8 devices in a mesh: dp: 2 (over z, y), tp: 4 (over x, core).
Axes of the slice: x: 2, y: 2, z: 1, core: 2. Of those that a mesh axis runs over, the one named last changes fastest.
Arguments:
- tokens: bfloat16 [4, 64, 4096], P('dp'), parts along dimension 0
- seq_lens: int32 [4], P('dp'), parts along dimension 0
- w_q: bfloat16 [4096, 4096], P(None, 'tp')
- w_k: bfloat16 [4096, 4096], P(None, 'tp')
- w_v: bfloat16 [4096, 4096], P(None, 'tp')
- w_o: bfloat16 [4096, 4096], P('tp')
- g_q: bfloat16 [4096], P('tp')
- g_k: bfloat16 [4096], P('tp')
- g_attn: bfloat16 [4096], replicated
- g_mlp: bfloat16 [4096], replicated
- w_gate: bfloat16 [4096, 11008], P(None, 'tp')
- w_up: bfloat16 [4096, 11008], P(None, 'tp')
- w_down: bfloat16 [11008, 4096], P('tp')
Outputs:
- output 1: bfloat16 [4, 64, 4096], P('dp'), parts along dimension 0
- output 2: bfloat16 [4, 32, 64, 128], P('dp', 'tp'), parts along dimension 0
- output 3: bfloat16 [4, 32, 64, 128], P('dp', 'tp'), parts along dimension 0
There are 2 independent parts. The reference program is written for one: setup_inputs(seed, part) draws one part's arguments, and reference() takes and returns one part's arrays. A program takes and returns all parts, laid end to end along the dimension named above; an argument that names none is the same for every part.
All inputs are finite; a program needn't handle non-finite values.
Results may differ from the reference program's by a relative error of at most 0.0144316.
Values are sent between devices in bfloat16 or wider.
A program may use at most 1 GiB of HBM per device.

```python
import jax
import jax.numpy as jnp
from jax import lax

PROMPTS = 2
SEQ_LEN = 64
D_MODEL = 4096
Q_HEADS = 32
KV_HEADS = 32
HEAD_DIM = 128
FF_DIM = 11008

ROPE_BASE = 500000.0
NORM_EPS = 1e-6


def setup_inputs(seed: int = 0, part: int = 0) -> dict:
    part_key = jax.random.fold_in(jax.random.key(seed), part)
    key_tok, key_len, key_slot = jax.random.split(part_key, 3)
    weight_keys = jax.random.split(jax.random.key(seed + 1), 13)
    q_width = Q_HEADS * HEAD_DIM
    kv_width = KV_HEADS * HEAD_DIM
    in_scale = D_MODEL ** -0.5
    tokens = jax.random.normal(key_tok, (PROMPTS, SEQ_LEN, D_MODEL), jnp.float32)
    seq_lens = jax.random.randint(key_len, (PROMPTS,), SEQ_LEN // 8, SEQ_LEN + 1, jnp.int32)
    full_slot = jax.random.randint(key_slot, (), 0, PROMPTS, jnp.int32)
    seq_lens = jnp.where(jnp.arange(PROMPTS) == full_slot, SEQ_LEN, seq_lens).astype(jnp.int32)
    q_head_scale = 2.0 ** jax.random.uniform(weight_keys[0], (Q_HEADS, 1), jnp.float32, -1.0, 1.0)
    k_head_scale = 2.0 ** jax.random.uniform(weight_keys[1], (KV_HEADS, 1), jnp.float32, -1.0, 1.0)
    w_q = (jax.random.normal(weight_keys[2], (D_MODEL, Q_HEADS, HEAD_DIM), jnp.float32) * q_head_scale * in_scale).reshape(D_MODEL, q_width)
    w_k = (jax.random.normal(weight_keys[3], (D_MODEL, KV_HEADS, HEAD_DIM), jnp.float32) * k_head_scale * in_scale).reshape(D_MODEL, kv_width)
    w_v = jax.random.normal(weight_keys[4], (D_MODEL, kv_width), jnp.float32) * in_scale
    w_o = jax.random.normal(weight_keys[5], (q_width, D_MODEL), jnp.float32) * q_width ** -0.5
    g_q = jax.random.uniform(weight_keys[6], (q_width,), jnp.float32, 0.5, 1.5)
    g_k = jax.random.uniform(weight_keys[7], (kv_width,), jnp.float32, 0.5, 1.5)
    g_attn = jax.random.uniform(weight_keys[8], (D_MODEL,), jnp.float32, 0.5, 1.5)
    g_mlp = jax.random.uniform(weight_keys[9], (D_MODEL,), jnp.float32, 0.5, 1.5)
    w_gate = jax.random.normal(weight_keys[10], (D_MODEL, FF_DIM), jnp.float32) * in_scale
    w_up = jax.random.normal(weight_keys[11], (D_MODEL, FF_DIM), jnp.float32) * in_scale
    w_down = jax.random.normal(weight_keys[12], (FF_DIM, D_MODEL), jnp.float32) * FF_DIM ** -0.5
    return dict(tokens=tokens.astype(jnp.bfloat16), seq_lens=seq_lens, w_q=w_q.astype(jnp.bfloat16), w_k=w_k.astype(jnp.bfloat16), w_v=w_v.astype(jnp.bfloat16), w_o=w_o.astype(jnp.bfloat16), g_q=g_q.astype(jnp.bfloat16), g_k=g_k.astype(jnp.bfloat16), g_attn=g_attn.astype(jnp.bfloat16), g_mlp=g_mlp.astype(jnp.bfloat16), w_gate=w_gate.astype(jnp.bfloat16), w_up=w_up.astype(jnp.bfloat16), w_down=w_down.astype(jnp.bfloat16))


def rope_tables(seq_len, head_dim):
    half_dim = head_dim // 2
    inv_freq = ROPE_BASE ** (-2.0 * jnp.arange(half_dim, dtype=jnp.float32) / head_dim)
    angles = jnp.arange(seq_len, dtype=jnp.float32)[:, None] * inv_freq[None, :]
    angles = jnp.concatenate([angles, angles], axis=-1)
    return jnp.cos(angles), jnp.sin(angles)


def apply_rope(vecs, cos_tab, sin_tab, head_axes):
    half_dim = vecs.shape[-1] // 2
    table_shape = (cos_tab.shape[0],) + (1,) * head_axes + (cos_tab.shape[1],)
    rotated = jnp.concatenate([-vecs[..., half_dim:], vecs[..., :half_dim]], axis=-1)
    return vecs * cos_tab.reshape(table_shape) + rotated * sin_tab.reshape(table_shape)


def rms_scale(vals):
    return lax.rsqrt(jnp.mean(vals * vals, axis=-1, keepdims=True) + NORM_EPS)


def post_norm(base, branch, gain):
    branch32 = branch.astype(jnp.float32)
    return (base.astype(jnp.float32) + branch32 * rms_scale(branch32) * gain.astype(jnp.float32)).astype(jnp.bfloat16)


def reference(tokens, seq_lens, w_q, w_k, w_v, w_o, g_q, g_k, g_attn, g_mlp, w_gate, w_up, w_down):
    group_size = Q_HEADS // KV_HEADS
    cos_tab, sin_tab = rope_tables(SEQ_LEN, HEAD_DIM)
    positions = jnp.arange(SEQ_LEN)
    causal = positions[None, :] <= positions[:, None]

    def one_prompt(item):
        prompt, length = item
        q_raw = jnp.dot(prompt, w_q, preferred_element_type=jnp.float32)
        k_raw = jnp.dot(prompt, w_k, preferred_element_type=jnp.float32)
        v_new = jnp.dot(prompt, w_v, preferred_element_type=jnp.float32).astype(jnp.bfloat16)
        q_norm = q_raw * rms_scale(q_raw) * g_q.astype(jnp.float32)
        k_norm = k_raw * rms_scale(k_raw) * g_k.astype(jnp.float32)
        queries = apply_rope(q_norm.reshape(SEQ_LEN, KV_HEADS, group_size, HEAD_DIM), cos_tab, sin_tab, 2).astype(jnp.bfloat16)
        keys_new = apply_rope(k_norm.reshape(SEQ_LEN, KV_HEADS, HEAD_DIM), cos_tab, sin_tab, 1).astype(jnp.bfloat16)
        v_heads = v_new.reshape(SEQ_LEN, KV_HEADS, HEAD_DIM)
        scores = jnp.einsum('sgrd,tgd->grst', queries.astype(jnp.float32), keys_new.astype(jnp.float32)) * HEAD_DIM ** -0.5
        allowed = causal & (positions[None, :] < length)
        scores = jnp.where(allowed, scores, -1e30)
        attn_probs = jax.nn.softmax(scores, axis=-1).astype(jnp.bfloat16)
        attn_out = jnp.einsum('grst,tgd->sgrd', attn_probs.astype(jnp.float32), v_heads.astype(jnp.float32)).astype(jnp.bfloat16)
        attn_proj = jnp.dot(attn_out.reshape(SEQ_LEN, Q_HEADS * HEAD_DIM), w_o, preferred_element_type=jnp.float32).astype(jnp.bfloat16)
        hidden = post_norm(prompt, attn_proj, g_attn)
        gate_pre = jnp.dot(hidden, w_gate, preferred_element_type=jnp.float32)
        up_proj = jnp.dot(hidden, w_up, preferred_element_type=jnp.float32)
        act_out = (jax.nn.silu(gate_pre) * up_proj).astype(jnp.bfloat16)
        mlp_out = jnp.dot(act_out, w_down, preferred_element_type=jnp.float32).astype(jnp.bfloat16)
        new_hidden = post_norm(hidden, mlp_out, g_mlp)
        return new_hidden, jnp.transpose(keys_new, (1, 0, 2)), jnp.transpose(v_heads, (1, 0, 2))

    out_hidden, k_cache, v_cache = lax.map(one_prompt, (tokens, seq_lens))
    return out_hidden, k_cache, v_cache
```

```python
import functools

import jax
import jax.numpy as jnp
import numpy as np
from jax import lax
from jax.experimental import pallas as pl
from jax.experimental.pallas import tpu as pltpu
from jax.sharding import PartitionSpec as P

HEAD_DIM = 128
ROPE_BASE = 500000.0
NORM_EPS = 1e-6

SEQ = 64
PROMPTS = 2
ROWS = SEQ * PROMPTS
HALF = ROWS // 2
D = 4096
QW = 1024
HEADS = QW // HEAD_DIM
FF = 2752
FFP = 2816
KC = 1024
CW = 512
NC = D // CW
TB = 256
NTB = FFP // TB
NS = 4
NT = 512

F32 = jnp.float32
BF16 = jnp.bfloat16
MESH = pl.DeviceIdType.MESH


def rope_tables():
    half = HEAD_DIM // 2
    inv_freq = ROPE_BASE ** (-2.0 * np.arange(half, dtype=np.float64) / HEAD_DIM)
    inv_freq = inv_freq.astype(np.float32)
    angles = np.arange(SEQ, dtype=np.float32)[:, None] * inv_freq[None, :]
    cos = np.cos(angles.astype(np.float64)).astype(np.float32)
    sin = np.sin(angles.astype(np.float64)).astype(np.float32)
    cos2 = np.concatenate([cos, cos], axis=1)
    sin2 = np.concatenate([-sin, sin], axis=1)
    return np.stack([np.tile(cos2, (PROMPTS, 1)), np.tile(sin2, (PROMPTS, 1))])


def dot(a, b):
    return jnp.dot(a, b, preferred_element_type=F32)


def kernel(lens, tok, wq, wk, wv, wo, gq_h, gk_h, ga_h, gm_h, wg, wu, wd, tab_h,
           y_h, kc_h, vc_h,
           stg, wgu, xh, acc, kout, vout, ob, part, d2d, xsend, xrecv, full, act,
           tab, gq, gk, ga, gm, ga32, gm32, st, st_recv, ssq,
           sem_in, sem_r, sem_g, sem_d, sem_out, st_s, st_r,
           d_s, d_r, x_s, x_r, a_s, a_r):
    me = lax.axis_index("tp")
    core = lax.rem(me, 2)
    partner = me + 1 - 2 * core
    cross = lax.rem(me + 2, 4)
    mine = pl.ds(pl.multiple_of(core * HALF, HALF), HALF)
    theirs = pl.ds(pl.multiple_of((1 - core) * HALF, HALF), HALF)
    local = pltpu.make_async_copy

    small = [(tok, xh), (tab_h, tab), (gq_h, gq), (gk_h, gk), (ga_h, ga), (gm_h, gm)]

    def in_copy(i):
        return local(small[i][0], small[i][1], sem_in.at[i])

    def slot(i):
        i = i % 8
        return wgu.at[1, pl.ds((i % 4) * KC, KC), pl.ds((i // 4) * KC, KC)]

    qkv = [wq, wk, wv]

    def stream(i):
        if i < 12:
            src = qkv[i // 4].at[pl.ds((i % 4) * KC, KC), :]
        else:
            src = wo.at[:, pl.ds((i - 12) * KC, KC)]
        return local(src, slot(i), sem_r.at[i])

    def gu_copy(w, n, s):
        rows = TB if n < NTB - 1 else FF - TB * (NTB - 1)
        return local(w.at[pl.ds(n * TB, rows), :], stg.at[s, pl.ds(0, rows), :], sem_g.at[s])

    def gu_start(j):
        s = lax.rem(j, NS)
        n = lax.rem(j, NTB)
        for m, w in enumerate((wg, wu)):
            @pl.when((j // NTB == m) & (n < NTB - 1))
            def _():
                rows = pl.ds(pl.multiple_of(n * TB, TB), TB)
                local(w.at[rows, :], stg.at[s], sem_g.at[s]).start()

            @pl.when((j // NTB == m) & (n == NTB - 1))
            def _():
                gu_copy(w, NTB - 1, s).start()

    def gu_wait(j):
        s = lax.rem(j, NS)
        n = lax.rem(j, NTB)

        @pl.when(n < NTB - 1)
        def _():
            gu_copy(wg, 0, s).wait()

        @pl.when(n == NTB - 1)
        def _():
            gu_copy(wg, NTB - 1, s).wait()

    def down_cols(c):
        return pl.ds(pl.multiple_of(c // 2 * CW, CW), CW)

    def down_copy(c):
        return local(wd.at[:, pl.ds(pl.multiple_of(c * CW, CW), CW)],
                     wgu.at[lax.rem(c, 2), pl.ds(0, FF), down_cols(c)], sem_d.at[c])

    in_copy(0).start()
    stream(0).start()
    for i in range(1, 6):
        in_copy(i).start()
    for i in range(1, 8):
        stream(i).start()

    barrier = pltpu.get_barrier_semaphore()
    for j in range(1, 4):
        pl.semaphore_signal(barrier, inc=1, device_id={"tp": lax.rem(me + j, 4)}, device_id_type=MESH)
    acc[...] = jnp.zeros_like(acc)
    st[...] = jnp.zeros_like(st)
    act[:, FF // 128 * 128:] = jnp.zeros((ROWS, FFP - FF // 128 * 128), BF16)
    in_copy(0).wait()

    def qkv_step(i):
        stream(i).wait()
        w, k = i // 4, i % 4
        acc[w] += dot(xh[:, k * KC:(k + 1) * KC], slot(i)[...])
        if i + 8 < 16:
            stream(i + 8).start()

    for i in range(8):
        qkv_step(i)
    for j in range(NS):
        gu_copy(wg, j, j).start()

    for w in range(2):
        t = jnp.zeros((ROWS, 128), F32)
        for h in range(HEADS):
            v = acc[w, :, h * 128:(h + 1) * 128]
            t = t + v * v
        st[w:w + 1, :] = jnp.sum(t.T, axis=0, keepdims=True)
    pl.semaphore_wait(barrier, 3)

    def st_copy(j):
        return pltpu.make_async_remote_copy(
            st, st_recv.at[j - 1], st_s.at[j - 1], st_r.at[j - 1],
            device_id={"tp": lax.rem(me + j, 4)}, device_id_type=MESH)

    for j in range(1, 4):
        st_copy(j).start()
    for i in range(8, 12):
        qkv_step(i)
    for i in range(1, 6):
        in_copy(i).wait()
    ga32[...] = ga[...].astype(F32)
    gm32[...] = gm[...].astype(F32)
    gq32, gk32 = gq[...].astype(F32), gk[...].astype(F32)
    for h in range(HEADS):
        vh = acc[2, :, h * 128:(h + 1) * 128].astype(BF16)
        vout[0, h] = vh[:SEQ]
        vout[1, h] = vh[SEQ:]
    v_out = local(vout, vc_h, sem_out.at[0])
    v_out.start()
    for j in range(1, 4):
        st_copy(j).wait()

    tot = st[...] + st_recv[0] + st_recv[1] + st_recv[2]
    rs = lax.rsqrt(tot * (1.0 / D) + NORM_EPS)
    rq = jnp.broadcast_to(rs[0:1, :], (ROWS, 128)).T
    rk = jnp.broadcast_to(rs[1:2, :], (ROWS, 128)).T
    cos, sin = tab[0], tab[1]

    def rope(v):
        return v * cos + pltpu.roll(v, 64, axis=1) * sin

    ri = lax.broadcasted_iota(jnp.int32, (ROWS, ROWS), 0)
    ci = lax.broadcasted_iota(jnp.int32, (ROWS, ROWS), 1)
    same = (ri < SEQ) == (ci < SEQ)
    limit = jnp.where(ci < SEQ, lens[0], lens[1] + SEQ)
    allowed = same & (ci <= ri) & (ci < limit)
    for h in range(HEADS):
        cols = slice(h * 128, (h + 1) * 128)
        qh = rope(acc[0, :, cols] * rq * gq32[h:h + 1]).astype(BF16)
        kh = rope(acc[1, :, cols] * rk * gk32[h:h + 1]).astype(BF16)
        kout[0, h] = kh[:SEQ]
        kout[1, h] = kh[SEQ:]
        s = lax.dot_general(qh, kh, (((1,), (1,)), ((), ())), preferred_element_type=F32) * HEAD_DIM ** -0.5
        s = jnp.where(allowed, s, -1e30)
        e = jnp.exp(s - jnp.max(s, axis=1, keepdims=True))
        p = (e / jnp.sum(e, axis=1, keepdims=True)).astype(BF16)
        vh = jnp.concatenate([vout[0, h], vout[1, h]], axis=0)
        ob[:, cols] = dot(p, vh).astype(BF16)
    k_out = local(kout, kc_h, sem_out.at[1])
    k_out.start()

    def d_copy(ph, c):
        return pltpu.make_async_remote_copy(
            part.at[c, theirs, :], d2d.at[c], d_s.at[ph, c], d_r.at[ph, c],
            device_id={"tp": partner}, device_id_type=MESH)

    def x_copy(ph, c):
        return pltpu.make_async_remote_copy(
            xsend.at[c], xrecv.at[ph, c], x_s.at[ph, c], x_r.at[ph, c],
            device_id={"tp": cross}, device_id_type=MESH)

    def cols_of(c):
        return pl.ds(pl.multiple_of(c * CW, CW), CW)

    def a_copy(ph, c):
        blk = full.at[mine, cols_of(c)]
        return pltpu.make_async_remote_copy(
            blk, blk, a_s.at[ph, c], a_r.at[ph, c],
            device_id={"tp": partner}, device_id_type=MESH)

    def put(ph, c, val):
        part[c] = val.astype(BF16)
        d_copy(ph, c).start()

    def relay(ph, c):
        d_copy(ph, c).wait()
        xsend[c] = (part[c, mine, :].astype(F32) + d2d[c].astype(F32)).astype(BF16)
        x_copy(ph, c).start()

    def add_sq(rows, c):
        v = full[rows, cols_of(c)].astype(F32)
        v = v * v
        t = v[:, 0:128]
        for q in range(1, CW // 128):
            t = t + v[:, q * 128:(q + 1) * 128]
        ssq[rows, :] += t

    def finish_own(ph, c):
        x_copy(ph, c).wait()
        s = xsend[c].astype(F32) + xrecv[ph, c].astype(F32)
        full[mine, cols_of(c)] = s.astype(BF16)
        a_copy(ph, c).start()
        add_sq(mine, c)

    def finish_other(ph, c):
        a_copy(ph, c).wait()
        add_sq(theirs, c)

    def norm(g32):
        rs = lax.rsqrt(jnp.sum(ssq[...], axis=1, keepdims=True) * (1.0 / D) + NORM_EPS)

        @pl.loop(0, NC)
        def _(c):
            for q in range(CW // 128):
                cols = pl.ds(pl.multiple_of(c * CW + q * 128, 128), 128)
                v = full[:, cols].astype(F32) * rs * g32[pl.ds(c * (CW // 128) + q, 1), :]
                xh[:, cols] = (xh[:, cols].astype(F32) + v).astype(BF16)

    ssq[...] = jnp.zeros_like(ssq)
    lag = 3
    for c in range(4):
        stream(12 + c).wait()
        for half in range(2):
            cc = 2 * c + half
            put(0, cc, dot(ob[...], slot(12 + c)[:, half * CW:(half + 1) * CW]))
            if cc >= lag:
                relay(0, cc - lag)

    @pl.loop(0, 2 * NTB)
    def _(j):
        gu_wait(j)
        s, m, n = lax.rem(j, NS), j // NTB, lax.rem(j, NTB)
        cols = pl.ds(pl.multiple_of(n * TB, TB), TB)
        wgu[m, :, cols] = stg[s].T

        @pl.when(j + NS < 2 * NTB)
        def _():
            gu_start(j + NS)

        @pl.when(j < lag)
        def _():
            relay(0, NC - lag + j)

        @pl.when((j >= 6) & (lax.rem(j, 2) == 0))
        def _():
            finish_own(0, (j - 6) // 2)

        @pl.when((j >= 7) & (lax.rem(j, 2) == 1))
        def _():
            finish_other(0, (j - 7) // 2)

    norm(ga32)

    def gate_up(start, width, keep):
        g = dot(xh[...], wgu[0, :, pl.ds(start, width)])
        u = dot(xh[...], wgu[1, :, pl.ds(start, width)])
        v = (g * jax.nn.sigmoid(g) * u).astype(BF16)
        act[:, pl.ds(start, keep)] = v[:, :keep]

    @pl.loop(0, FF // NT)
    def _(n):
        gate_up(pl.multiple_of(n * NT, NT), NT, NT)

        @pl.when(n < NC // 2)
        def _():
            down_copy(2 * n).start()
            down_copy(2 * n + 1).start()

    tail = FF // NT * NT
    gate_up(tail, FFP - tail, FF - tail)
    ssq[...] = jnp.zeros_like(ssq)

    lag2 = 2

    @pl.loop(0, NC)
    def _(c):
        down_copy(c).wait()
        put(1, c, dot(act[...], wgu[lax.rem(c, 2), :FFP, down_cols(c)]))

        @pl.when(c >= lag2)
        def _():
            relay(1, c - lag2)

    for cc in range(NC - lag2, NC):
        relay(1, cc)

    @pl.loop(0, NC)
    def _(c):
        finish_own(1, c)

        @pl.when(c > 0)
        def _():
            finish_other(1, c - 1)

    finish_other(1, NC - 1)
    norm(gm32)
    y_out = local(xh, y_h, sem_out.at[2])
    y_out.start()
    y_out.wait()
    v_out.wait()
    k_out.wait()


def solution(mesh):
    tables = rope_tables()

    def local_layer(tokens, seq_lens, w_q, w_k, w_v, w_o, g_q, g_k, g_attn, g_mlp, w_gate, w_up, w_down):
        anyspace = pl.BlockSpec(memory_space=pl.ANY)
        dma = pltpu.SemaphoreType.DMA
        y, kc, vc = pl.pallas_call(
            kernel,
            out_shape=(
                jax.ShapeDtypeStruct((ROWS, D), BF16),
                jax.ShapeDtypeStruct((PROMPTS, HEADS, SEQ, HEAD_DIM), BF16),
                jax.ShapeDtypeStruct((PROMPTS, HEADS, SEQ, HEAD_DIM), BF16),
            ),
            in_specs=[pl.BlockSpec(memory_space=pltpu.SMEM)] + [anyspace] * 13,
            out_specs=(anyspace,) * 3,
            scratch_shapes=[
                pltpu.VMEM((NS, TB, D), BF16),
                pltpu.VMEM((2, D, FFP), BF16),
                pltpu.VMEM((ROWS, D), BF16),
                pltpu.VMEM((3, ROWS, QW), F32),
                pltpu.VMEM((PROMPTS, HEADS, SEQ, HEAD_DIM), BF16),
                pltpu.VMEM((PROMPTS, HEADS, SEQ, HEAD_DIM), BF16),
                pltpu.VMEM((ROWS, QW), BF16),
                pltpu.VMEM((NC, ROWS, CW), BF16),
                pltpu.VMEM((NC, HALF, CW), BF16),
                pltpu.VMEM((NC, HALF, CW), BF16),
                pltpu.VMEM((2, NC, HALF, CW), BF16),
                pltpu.VMEM((ROWS, D), BF16),
                pltpu.VMEM((ROWS, FFP), BF16),
                pltpu.VMEM((2, ROWS, HEAD_DIM), F32),
                pltpu.VMEM((QW // 128, 128), BF16),
                pltpu.VMEM((QW // 128, 128), BF16),
                pltpu.VMEM((D // 128, 128), BF16),
                pltpu.VMEM((D // 128, 128), BF16),
                pltpu.VMEM((D // 128, 128), F32),
                pltpu.VMEM((D // 128, 128), F32),
                pltpu.VMEM((8, 128), F32),
                pltpu.VMEM((3, 8, 128), F32),
                pltpu.VMEM((ROWS, 128), F32),
                dma((6,)), dma((16,)), dma((NS,)), dma((NC,)), dma((3,)), dma((3,)), dma((3,)),
                dma((2, NC)), dma((2, NC)), dma((2, NC)), dma((2, NC)), dma((2, NC)), dma((2, NC)),
            ],
            compiler_params=pltpu.CompilerParams(
                collective_id=0, has_side_effects=True, vmem_limit_bytes=67043328),
            name="layer",
        )(seq_lens, tokens.reshape(ROWS, D), w_q, w_k, w_v, w_o,
          g_q.reshape(-1, 128), g_k.reshape(-1, 128), g_attn.reshape(-1, 128), g_mlp.reshape(-1, 128),
          w_gate.T, w_up.T, w_down, jnp.asarray(tables))
        return y.reshape(tokens.shape), kc, vc

    return jax.shard_map(local_layer, mesh=mesh, in_specs=(P('dp', None, None), P('dp'), P(None, 'tp'), P(None, 'tp'), P(None, 'tp'), P('tp', None), P('tp'), P('tp'), P(), P(), P(None, 'tp'), P(None, 'tp'), P('tp', None)), out_specs=(P('dp', None, None), P('dp', 'tp', None, None), P('dp', 'tp', None, None)), check_vma=False)
```

```python
import functools

import jax
import jax.numpy as jnp
import numpy as np
from jax import lax
from jax.experimental import pallas as pl
from jax.experimental.pallas import tpu as pltpu
from jax.sharding import PartitionSpec as P

HEAD_DIM = 128
ROPE_BASE = 500000.0
NORM_EPS = 1e-6

SEQ = 64
PROMPTS = 2
ROWS = SEQ * PROMPTS
HALF = ROWS // 2
D = 4096
QW = 1024
HEADS = QW // HEAD_DIM
FF = 2752
FFP = 2816
KC = 1024
CW = 512
NC = D // CW
TB = 256
NTB = FFP // TB
NS = 4
DEPTH = 4
NT = 512

VMEM_LIMIT = 62 * 2**20

F32 = jnp.float32
BF16 = jnp.bfloat16
MESH = pl.DeviceIdType.MESH


def rope_tables():
    half = HEAD_DIM // 2
    inv_freq = ROPE_BASE ** (-2.0 * np.arange(half, dtype=np.float64) / HEAD_DIM)
    inv_freq = inv_freq.astype(np.float32)
    angles = np.arange(SEQ, dtype=np.float32)[:, None] * inv_freq[None, :]
    cos = np.cos(angles.astype(np.float64)).astype(np.float32)
    sin = np.sin(angles.astype(np.float64)).astype(np.float32)
    cos2 = np.concatenate([cos, cos], axis=1)
    sin2 = np.concatenate([-sin, sin], axis=1)
    return np.stack([np.tile(cos2, (PROMPTS, 1)), np.tile(sin2, (PROMPTS, 1))])


def dot(a, b):
    return jnp.dot(a, b, preferred_element_type=F32)


_cur = []


def _ph(name):
    if _cur:
        _cur.pop().__exit__(None, None, None)
    if name != 'end':
        sc = jax.named_scope(name)
        sc.__enter__()
        _cur.append(sc)


def kernel(lens, tok, wq, wk, wv, wo, gq_h, gk_h, ga_h, gm_h, wg, wu, wd, tab_h,
           xh, kout, vout,
           stg, wgu, acc, ob, part, d2d, xsend, xrecv, full, act,
           tab, gq, gk, ga, gm, ga32, gm32, st, st_recv, ssq,
           sem_in, sem_r, sem_g, sem_d, st_s, st_r,
           d_s, d_r, x_s, x_r, a_s, a_r):
    me = lax.axis_index("tp")
    core = lax.rem(me, 2)
    partner = me + 1 - 2 * core
    cross = lax.rem(me + 2, 4)
    mine = pl.ds(pl.multiple_of(core * HALF, HALF), HALF)
    theirs = pl.ds(pl.multiple_of((1 - core) * HALF, HALF), HALF)
    local = pltpu.make_async_copy

    small = [(tok, xh), (tab_h, tab), (gq_h, gq), (gk_h, gk), (ga_h, ga), (gm_h, gm)]

    def in_copy(i):
        return local(small[i][0], small[i][1], sem_in.at[i])

    def slot(i):
        i = i % 8
        return wgu.at[1, pl.ds((i % 4) * KC, KC), pl.ds((i // 4) * KC, KC)]

    qkv = [wq, wk, wv]

    def stream(i):
        if i < 12:
            src = qkv[i // 4].at[pl.ds((i % 4) * KC, KC), :]
        else:
            src = wo.at[:, pl.ds((i - 12) * KC, KC)]
        return local(src, slot(i), sem_r.at[i])

    def gu_copy(w, n, s):
        rows = TB if n < NTB - 1 else FF - TB * (NTB - 1)
        return local(w.at[pl.ds(n * TB, rows), :], stg.at[s, pl.ds(0, rows), :], sem_g.at[s])

    def gu_start(j):
        s = lax.rem(j, NS)
        n = lax.rem(j, NTB)
        for m, w in enumerate((wg, wu)):
            @pl.when((j // NTB == m) & (n < NTB - 1))
            def _():
                rows = pl.ds(pl.multiple_of(n * TB, TB), TB)
                local(w.at[rows, :], stg.at[s], sem_g.at[s]).start()

            @pl.when((j // NTB == m) & (n == NTB - 1))
            def _():
                gu_copy(w, NTB - 1, s).start()

    def gu_wait(j):
        s = lax.rem(j, NS)
        n = lax.rem(j, NTB)

        @pl.when(n < NTB - 1)
        def _():
            gu_copy(wg, 0, s).wait()

        @pl.when(n == NTB - 1)
        def _():
            gu_copy(wg, NTB - 1, s).wait()

    def down_cols(c):
        return pl.ds(pl.multiple_of(c // 2 * CW, CW), CW)

    def down_copy(c):
        return local(wd.at[:, pl.ds(pl.multiple_of(c * CW, CW), CW)],
                     wgu.at[lax.rem(c, 2), pl.ds(0, FF), down_cols(c)], sem_d.at[c])

    _ph('init')
    in_copy(0).start()
    stream(0).start()
    for i in range(1, 6):
        in_copy(i).start()
    for i in range(1, DEPTH):
        stream(i).start()

    barrier = pltpu.get_barrier_semaphore()
    for j in range(1, 4):
        pl.semaphore_signal(barrier, inc=1, device_id={"tp": lax.rem(me + j, 4)}, device_id_type=MESH)
    acc[...] = jnp.zeros_like(acc)
    st[...] = jnp.zeros_like(st)
    act[:, FF // 128 * 128:] = jnp.zeros((ROWS, FFP - FF // 128 * 128), BF16)
    _ph('wait_x')
    in_copy(0).wait()

    def qkv_step(i):
        stream(i).wait()
        w, k = i // 4, i % 4
        acc[w] += dot(xh[:, k * KC:(k + 1) * KC], slot(i)[...])
        if i + DEPTH < 16:
            stream(i + DEPTH).start()

    _ph('qk')
    for i in range(8):
        qkv_step(i)
    _ph('ssq_send')
    for w in range(2):
        t = jnp.zeros((ROWS, 128), F32)
        for h in range(HEADS):
            v = acc[w, :, h * 128:(h + 1) * 128]
            t = t + v * v
        st[w:w + 1, :] = jnp.sum(t.T, axis=0, keepdims=True)
    pl.semaphore_wait(barrier, 3)

    def st_copy(j):
        return pltpu.make_async_remote_copy(
            st, st_recv.at[j - 1], st_s.at[j - 1], st_r.at[j - 1],
            device_id={"tp": lax.rem(me + j, 4)}, device_id_type=MESH)

    for j in range(1, 4):
        st_copy(j).start()
    _ph('v')
    for i in range(8, 12):
        qkv_step(i)
    for j in range(NS):
        gu_copy(wg, j, j).start()
    _ph('vout')
    for i in range(1, 6):
        in_copy(i).wait()
    ga32[...] = ga[...].astype(F32)
    gm32[...] = gm[...].astype(F32)
    gq32, gk32 = gq[...].astype(F32), gk[...].astype(F32)
    for h in range(HEADS):
        vh = acc[2, :, h * 128:(h + 1) * 128].astype(BF16)
        vout[0, h] = vh[:SEQ]
        vout[1, h] = vh[SEQ:]
    _ph('st_wait')
    for j in range(1, 4):
        st_copy(j).wait()

    _ph('attn')
    tot = st[...] + st_recv[0] + st_recv[1] + st_recv[2]
    rs = lax.rsqrt(tot * (1.0 / D) + NORM_EPS)
    rq = jnp.broadcast_to(rs[0:1, :], (ROWS, 128)).T
    rk = jnp.broadcast_to(rs[1:2, :], (ROWS, 128)).T
    cos, sin = tab[0], tab[1]

    def rope(v):
        return v * cos + pltpu.roll(v, 64, axis=1) * sin

    ri = lax.broadcasted_iota(jnp.int32, (ROWS, ROWS), 0)
    ci = lax.broadcasted_iota(jnp.int32, (ROWS, ROWS), 1)
    same = (ri < SEQ) == (ci < SEQ)
    limit = jnp.where(ci < SEQ, lens[0], lens[1] + SEQ)
    allowed = same & (ci <= ri) & (ci < limit)
    for h in range(HEADS):
        _ph('head')
        cols = slice(h * 128, (h + 1) * 128)
        qh = rope(acc[0, :, cols] * rq * gq32[h:h + 1]).astype(BF16)
        kh = rope(acc[1, :, cols] * rk * gk32[h:h + 1]).astype(BF16)
        kout[0, h] = kh[:SEQ]
        kout[1, h] = kh[SEQ:]
        s = lax.dot_general(qh, kh, (((1,), (1,)), ((), ())), preferred_element_type=F32) * HEAD_DIM ** -0.5
        s = jnp.where(allowed, s, -1e30)
        e = jnp.exp(s - jnp.max(s, axis=1, keepdims=True))
        p = (e / jnp.sum(e, axis=1, keepdims=True)).astype(BF16)
        vh = jnp.concatenate([vout[0, h], vout[1, h]], axis=0)
        ob[:, cols] = dot(p, vh).astype(BF16)

    def d_copy(ph, c):
        return pltpu.make_async_remote_copy(
            part.at[c, theirs, :], d2d.at[c], d_s.at[ph, c], d_r.at[ph, c],
            device_id={"tp": partner}, device_id_type=MESH)

    def x_copy(ph, c):
        return pltpu.make_async_remote_copy(
            xsend.at[c], xrecv.at[ph, c], x_s.at[ph, c], x_r.at[ph, c],
            device_id={"tp": cross}, device_id_type=MESH)

    def cols_of(c):
        return pl.ds(pl.multiple_of(c * CW, CW), CW)

    def a_copy(ph, c):
        blk = full.at[mine, cols_of(c)]
        return pltpu.make_async_remote_copy(
            blk, blk, a_s.at[ph, c], a_r.at[ph, c],
            device_id={"tp": partner}, device_id_type=MESH)

    def put(ph, c, val):
        part[c] = val.astype(BF16)
        d_copy(ph, c).start()

    def relay(ph, c):
        d_copy(ph, c).wait()
        xsend[c] = (part[c, mine, :].astype(F32) + d2d[c].astype(F32)).astype(BF16)
        x_copy(ph, c).start()

    def add_sq(rows, c):
        v = full[rows, cols_of(c)].astype(F32)
        v = v * v
        t = v[:, 0:128]
        for q in range(1, CW // 128):
            t = t + v[:, q * 128:(q + 1) * 128]
        ssq[rows, :] += t

    def finish_own(ph, c):
        x_copy(ph, c).wait()
        s = xsend[c].astype(F32) + xrecv[ph, c].astype(F32)
        full[mine, cols_of(c)] = s.astype(BF16)
        a_copy(ph, c).start()
        add_sq(mine, c)

    def finish_other(ph, c):
        a_copy(ph, c).wait()
        add_sq(theirs, c)

    def norm(g32):
        rs = lax.rsqrt(jnp.sum(ssq[...], axis=1, keepdims=True) * (1.0 / D) + NORM_EPS)

        @pl.loop(0, NC)
        def _(c):
            for q in range(CW // 128):
                cols = pl.ds(pl.multiple_of(c * CW + q * 128, 128), 128)
                v = full[:, cols].astype(F32) * rs * g32[pl.ds(c * (CW // 128) + q, 1), :]
                xh[:, cols] = (xh[:, cols].astype(F32) + v).astype(BF16)

    _ph('wo')
    ssq[...] = jnp.zeros_like(ssq)
    lag = 3
    for c in range(4):
        _ph('wo_wait')
        stream(12 + c).wait()
        for half in range(2):
            cc = 2 * c + half
            _ph('wo_dot')
            put(0, cc, dot(ob[...], slot(12 + c)[:, half * CW:(half + 1) * CW]))
            _ph('wo_relay')
            if cc >= lag:
                relay(0, cc - lag)

    _ph('xpose')
    @pl.loop(0, 2 * NTB)
    def _(j):
        gu_wait(j)
        s, m, n = lax.rem(j, NS), j // NTB, lax.rem(j, NTB)
        cols = pl.ds(pl.multiple_of(n * TB, TB), TB)
        wgu[m, :, cols] = stg[s].T

        @pl.when(j + NS < 2 * NTB)
        def _():
            gu_start(j + NS)

        @pl.when(j < lag)
        def _():
            relay(0, NC - lag + j)

        @pl.when((j >= 6) & (lax.rem(j, 2) == 0))
        def _():
            finish_own(0, (j - 6) // 2)

        @pl.when((j >= 7) & (lax.rem(j, 2) == 1))
        def _():
            finish_other(0, (j - 7) // 2)

    _ph('norm1')
    norm(ga32)

    _ph('gate_up')
    def gate_up(start, width, keep):
        g = dot(xh[...], wgu[0, :, pl.ds(start, width)])
        u = dot(xh[...], wgu[1, :, pl.ds(start, width)])
        v = (g * jax.nn.sigmoid(g) * u).astype(BF16)
        act[:, pl.ds(start, keep)] = v[:, :keep]

    @pl.loop(0, FF // NT)
    def _(n):
        gate_up(pl.multiple_of(n * NT, NT), NT, NT)

        @pl.when(n < NC // 2)
        def _():
            down_copy(2 * n).start()
            down_copy(2 * n + 1).start()

    tail = FF // NT * NT
    gate_up(tail, FFP - tail, FF - tail)
    ssq[...] = jnp.zeros_like(ssq)

    _ph('down')
    lag2 = 2

    @pl.loop(0, NC)
    def _(c):
        down_copy(c).wait()
        put(1, c, dot(act[...], wgu[lax.rem(c, 2), :FFP, down_cols(c)]))

        @pl.when(c >= lag2)
        def _():
            relay(1, c - lag2)

    _ph('relay_tail')
    for cc in range(NC - lag2, NC):
        relay(1, cc)

    _ph('finish2')
    @pl.loop(0, NC)
    def _(c):
        finish_own(1, c)

        @pl.when(c > 0)
        def _():
            finish_other(1, c - 1)

    finish_other(1, NC - 1)
    _ph('norm2')
    norm(gm32)
    _ph('end')


def solution(mesh):
    tables = rope_tables()

    def local_layer(tokens, seq_lens, w_q, w_k, w_v, w_o, g_q, g_k, g_attn, g_mlp, w_gate, w_up, w_down):
        vmem = pl.BlockSpec(memory_space=pltpu.VMEM)
        anyspace = pl.BlockSpec(memory_space=pl.ANY)
        dma = pltpu.SemaphoreType.DMA
        y, kc, vc = pl.pallas_call(
            kernel,
            out_shape=(
                pltpu.VMEM((ROWS, D), BF16),
                pltpu.VMEM((PROMPTS, HEADS, SEQ, HEAD_DIM), BF16),
                pltpu.VMEM((PROMPTS, HEADS, SEQ, HEAD_DIM), BF16),
            ),
            in_specs=[pl.BlockSpec(memory_space=pltpu.SMEM)] + [anyspace] * 13,
            out_specs=(vmem,) * 3,
            scratch_shapes=[
                pltpu.VMEM((NS, TB, D), BF16),
                pltpu.VMEM((2, D, FFP), BF16),
                pltpu.VMEM((3, ROWS, QW), F32),
                pltpu.VMEM((ROWS, QW), BF16),
                pltpu.VMEM((NC, ROWS, CW), BF16),
                pltpu.VMEM((NC, HALF, CW), BF16),
                pltpu.VMEM((NC, HALF, CW), BF16),
                pltpu.VMEM((2, NC, HALF, CW), BF16),
                pltpu.VMEM((ROWS, D), BF16),
                pltpu.VMEM((ROWS, FFP), BF16),
                pltpu.VMEM((2, ROWS, HEAD_DIM), F32),
                pltpu.VMEM((QW // 128, 128), BF16),
                pltpu.VMEM((QW // 128, 128), BF16),
                pltpu.VMEM((D // 128, 128), BF16),
                pltpu.VMEM((D // 128, 128), BF16),
                pltpu.VMEM((D // 128, 128), F32),
                pltpu.VMEM((D // 128, 128), F32),
                pltpu.VMEM((8, 128), F32),
                pltpu.VMEM((3, 8, 128), F32),
                pltpu.VMEM((ROWS, 128), F32),
                dma((6,)), dma((16,)), dma((NS,)), dma((NC,)), dma((3,)), dma((3,)),
                dma((2, NC)), dma((2, NC)), dma((2, NC)), dma((2, NC)), dma((2, NC)), dma((2, NC)),
            ],
            compiler_params=pltpu.CompilerParams(
                collective_id=0, has_side_effects=True, vmem_limit_bytes=VMEM_LIMIT),
            name="layer",
        )(seq_lens, tokens.reshape(ROWS, D), w_q, w_k, w_v, w_o,
          g_q.reshape(-1, 128), g_k.reshape(-1, 128), g_attn.reshape(-1, 128), g_mlp.reshape(-1, 128),
          w_gate.T, w_up.T, w_down, jnp.asarray(tables))
        return y.reshape(tokens.shape), kc, vc

    return jax.shard_map(local_layer, mesh=mesh, in_specs=(P('dp', None, None), P('dp'), P(None, 'tp'), P(None, 'tp'), P(None, 'tp'), P('tp', None), P('tp'), P('tp'), P(), P(), P(None, 'tp'), P(None, 'tp'), P('tp', None)), out_specs=(P('dp', None, None), P('dp', 'tp', None, None), P('dp', 'tp', None, None)), check_vma=False)
```

```python
import functools

import jax
import jax.numpy as jnp
import numpy as np
from jax import lax
from jax.experimental import pallas as pl
from jax.experimental.pallas import tpu as pltpu
from jax.sharding import PartitionSpec as P

HEAD_DIM = 128
ROPE_BASE = 500000.0
NORM_EPS = 1e-6

SEQ = 64
PROMPTS = 2
ROWS = SEQ * PROMPTS
HALF = ROWS // 2
D = 4096
QW = 1024
HEADS = QW // HEAD_DIM
FF = 2752
FFP = 2816
KC = 1024
CW = 512
NC = D // CW
TB = 256
NTB = FFP // TB
NS = 4
DEPTH = 4
NT = 512

VMEM_LIMIT = 62 * 2**20

F32 = jnp.float32
BF16 = jnp.bfloat16
MESH = pl.DeviceIdType.MESH


def rope_tables():
    half = HEAD_DIM // 2
    inv_freq = ROPE_BASE ** (-2.0 * np.arange(half, dtype=np.float64) / HEAD_DIM)
    inv_freq = inv_freq.astype(np.float32)
    angles = np.arange(SEQ, dtype=np.float32)[:, None] * inv_freq[None, :]
    cos = np.cos(angles.astype(np.float64)).astype(np.float32)
    sin = np.sin(angles.astype(np.float64)).astype(np.float32)
    cos2 = np.concatenate([cos, cos], axis=1)
    sin2 = np.concatenate([-sin, sin], axis=1)
    return np.stack([np.tile(cos2, (PROMPTS, 1)), np.tile(sin2, (PROMPTS, 1))])


def dot(a, b):
    return jnp.dot(a, b, preferred_element_type=F32)


def dot_t(a, b):
    return lax.dot_general(a, b, (((1,), (1,)), ((), ())), preferred_element_type=F32)


_cur = []


def _ph(name):
    if _cur:
        _cur.pop().__exit__(None, None, None)
    if name != 'end':
        sc = jax.named_scope(name)
        sc.__enter__()
        _cur.append(sc)


def kernel(lens, tok, wq, wk, wv, wo, gq_h, gk_h, ga_h, gm_h, wg, wu, wd, tab_h,
           xh, kout, vout,
           stg, wgu, acc, ob, part, d2d, xsend, xrecv, full, act,
           tab, gq, gk, ga, gm, ga32, gm32, st, st_recv, ssq, eye, qb, pb,
           sem_in, sem_r, sem_g, sem_d, st_s, st_r,
           d_s, d_r, x_s, x_r, a_s, a_r):
    me = lax.axis_index("tp")
    core = lax.rem(me, 2)
    partner = me + 1 - 2 * core
    cross = lax.rem(me + 2, 4)
    mine = pl.ds(pl.multiple_of(core * HALF, HALF), HALF)
    theirs = pl.ds(pl.multiple_of((1 - core) * HALF, HALF), HALF)
    local = pltpu.make_async_copy

    small = [(tok, xh), (tab_h, tab), (gq_h, gq), (gk_h, gk), (ga_h, ga), (gm_h, gm)]

    def in_copy(i):
        return local(small[i][0], small[i][1], sem_in.at[i])

    def slot(i):
        i = i % 8
        return wgu.at[1, pl.ds((i % 4) * KC, KC), pl.ds((i // 4) * KC, KC)]

    qkv = [wq, wk, wv]

    def stream(i):
        if i < 12:
            src = qkv[i // 4].at[pl.ds((i % 4) * KC, KC), :]
        else:
            src = wo.at[:, pl.ds((i - 12) * KC, KC)]
        return local(src, slot(i), sem_r.at[i])

    def gu_copy(w, n, s):
        rows = TB if n < NTB - 1 else FF - TB * (NTB - 1)
        return local(w.at[pl.ds(n * TB, rows), :], stg.at[s, pl.ds(0, rows), :], sem_g.at[s])

    def gu_start(j):
        s = lax.rem(j, NS)
        n = lax.rem(j, NTB)
        for m, w in enumerate((wg, wu)):
            @pl.when((j // NTB == m) & (n < NTB - 1))
            def _():
                rows = pl.ds(pl.multiple_of(n * TB, TB), TB)
                local(w.at[rows, :], stg.at[s], sem_g.at[s]).start()

            @pl.when((j // NTB == m) & (n == NTB - 1))
            def _():
                gu_copy(w, NTB - 1, s).start()

    def gu_wait(j):
        s = lax.rem(j, NS)
        n = lax.rem(j, NTB)

        @pl.when(n < NTB - 1)
        def _():
            gu_copy(wg, 0, s).wait()

        @pl.when(n == NTB - 1)
        def _():
            gu_copy(wg, NTB - 1, s).wait()

    def down_cols(c):
        return pl.ds(pl.multiple_of(c // 2 * CW, CW), CW)

    def down_copy(c):
        return local(wd.at[:, pl.ds(pl.multiple_of(c * CW, CW), CW)],
                     wgu.at[lax.rem(c, 2), pl.ds(0, FF), down_cols(c)], sem_d.at[c])

    _ph('init')
    in_copy(0).start()
    stream(0).start()
    for i in range(1, 6):
        in_copy(i).start()
    for i in range(1, DEPTH):
        stream(i).start()

    barrier = pltpu.get_barrier_semaphore()
    for j in range(1, 4):
        pl.semaphore_signal(barrier, inc=1, device_id={"tp": lax.rem(me + j, 4)}, device_id_type=MESH)
    acc[...] = jnp.zeros_like(acc)
    st[...] = jnp.zeros_like(st)
    er = lax.broadcasted_iota(jnp.int32, (TB, TB), 0)
    ec = lax.broadcasted_iota(jnp.int32, (TB, TB), 1)
    eye[...] = (er == ec).astype(F32).astype(BF16)
    act[:, FF // 128 * 128:] = jnp.zeros((ROWS, FFP - FF // 128 * 128), BF16)
    _ph('wait_x')
    in_copy(0).wait()

    def qkv_step(i):
        stream(i).wait()
        w, k = i // 4, i % 4
        acc[w] += dot(xh[:, k * KC:(k + 1) * KC], slot(i)[...])
        if i + DEPTH < 16:
            stream(i + DEPTH).start()

    _ph('qk')
    for i in range(8):
        qkv_step(i)
    _ph('ssq_send')
    for w in range(2):
        t = jnp.zeros((ROWS, 128), F32)
        for h in range(HEADS):
            v = acc[w, :, h * 128:(h + 1) * 128]
            t = t + v * v
        st[w:w + 1, :] = jnp.sum(t.T, axis=0, keepdims=True)
    pl.semaphore_wait(barrier, 3)

    def st_copy(j):
        return pltpu.make_async_remote_copy(
            st, st_recv.at[j - 1], st_s.at[j - 1], st_r.at[j - 1],
            device_id={"tp": lax.rem(me + j, 4)}, device_id_type=MESH)

    for j in range(1, 4):
        st_copy(j).start()
    _ph('v')
    for i in range(8, 12):
        qkv_step(i)
    for j in range(NS):
        gu_copy(wg, j, j).start()
    _ph('vout')
    for i in range(1, 6):
        in_copy(i).wait()
    ga32[...] = ga[...].astype(F32)
    gm32[...] = gm[...].astype(F32)
    gq32, gk32 = gq[...].astype(F32), gk[...].astype(F32)
    for h in range(HEADS):
        vh = acc[2, :, h * 128:(h + 1) * 128].astype(BF16)
        vout[0, h] = vh[:SEQ]
        vout[1, h] = vh[SEQ:]
    _ph('st_wait')
    for j in range(1, 4):
        st_copy(j).wait()

    _ph('attn')
    tot = st[...] + st_recv[0] + st_recv[1] + st_recv[2]
    rs = lax.rsqrt(tot * (1.0 / D) + NORM_EPS)
    rq = jnp.broadcast_to(rs[0:1, :], (ROWS, 128)).T
    rk = jnp.broadcast_to(rs[1:2, :], (ROWS, 128)).T
    cos, sin = tab[0], tab[1]

    def rope(v):
        return v * cos + pltpu.roll(v, 64, axis=1) * sin

    ri = lax.broadcasted_iota(jnp.int32, (ROWS, ROWS), 0)
    ci = lax.broadcasted_iota(jnp.int32, (ROWS, ROWS), 1)
    same = (ri < SEQ) == (ci < SEQ)
    limit = jnp.where(ci < SEQ, lens[0], lens[1] + SEQ)
    allowed = same & (ci <= ri) & (ci < limit)
    for h in range(HEADS):
        cols = slice(h * 128, (h + 1) * 128)
        qb[h] = rope(acc[0, :, cols] * rq * gq32[h:h + 1]).astype(BF16)
        kh = rope(acc[1, :, cols] * rk * gk32[h:h + 1]).astype(BF16)
        kout[0, h] = kh[:SEQ]
        kout[1, h] = kh[SEQ:]
    for h in range(HEADS):
        kh = jnp.concatenate([kout[0, h], kout[1, h]], axis=0)
        s = jnp.where(allowed, dot_t(qb[h], kh) * HEAD_DIM ** -0.5, -1e30)
        e = jnp.exp(s - jnp.max(s, axis=1, keepdims=True))
        pb[h] = (e / jnp.sum(e, axis=1, keepdims=True)).astype(BF16)
    for h in range(HEADS):
        vh = jnp.concatenate([vout[0, h], vout[1, h]], axis=0)
        ob[:, h * 128:(h + 1) * 128] = dot(pb[h], vh).astype(BF16)

    def d_copy(ph, c):
        return pltpu.make_async_remote_copy(
            part.at[c, theirs, :], d2d.at[c], d_s.at[c], d_r.at[c],
            device_id={"tp": partner}, device_id_type=MESH)

    def x_copy(ph, c):
        return pltpu.make_async_remote_copy(
            xsend.at[c], xrecv.at[ph, c], x_s.at[c], x_r.at[ph, c],
            device_id={"tp": cross}, device_id_type=MESH)

    def cols_of(c):
        return pl.ds(pl.multiple_of(c * CW, CW), CW)

    def a_copy(ph, c):
        blk = full.at[mine, cols_of(c)]
        return pltpu.make_async_remote_copy(
            blk, blk, a_s.at[c], a_r.at[c],
            device_id={"tp": partner}, device_id_type=MESH)

    def put(ph, c, val):
        part[c] = val.astype(BF16)
        d_copy(ph, c).start()

    def relay(ph, c):
        d_copy(ph, c).wait()
        xsend[c] = (part[c, mine, :].astype(F32) + d2d[c].astype(F32)).astype(BF16)
        x_copy(ph, c).start()

    def add_sq(rows, c):
        v = full[rows, cols_of(c)].astype(F32)
        v = v * v
        t = v[:, 0:128]
        for q in range(1, CW // 128):
            t = t + v[:, q * 128:(q + 1) * 128]
        ssq[rows, :] += t

    def finish_own(ph, c):
        x_copy(ph, c).wait()
        s = xsend[c].astype(F32) + xrecv[ph, c].astype(F32)
        full[mine, cols_of(c)] = s.astype(BF16)
        a_copy(ph, c).start()
        add_sq(mine, c)

    def finish_other(ph, c):
        a_copy(ph, c).wait()
        add_sq(theirs, c)

    def norm(g32):
        rs = lax.rsqrt(jnp.sum(ssq[...], axis=1, keepdims=True) * (1.0 / D) + NORM_EPS)

        @pl.loop(0, NC)
        def _(c):
            for q in range(CW // 128):
                cols = pl.ds(pl.multiple_of(c * CW + q * 128, 128), 128)
                v = full[:, cols].astype(F32) * rs * g32[pl.ds(c * (CW // 128) + q, 1), :]
                xh[:, cols] = (xh[:, cols].astype(F32) + v).astype(BF16)

    _ph('wo')
    ssq[...] = jnp.zeros_like(ssq)
    lag = 2
    for c in range(4):
        stream(12 + c).wait()
        for half in range(2):
            cc = 2 * c + half
            put(0, cc, dot(ob[...], slot(12 + c)[:, half * CW:(half + 1) * CW]))
            if cc >= lag:
                relay(0, cc - lag)

    _ph('xpose')
    @pl.loop(0, 2 * NTB)
    def _(j):
        gu_wait(j)
        s, m, n = lax.rem(j, NS), j // NTB, lax.rem(j, NTB)
        cols = pl.ds(pl.multiple_of(n * TB, TB), TB)
        for k in range(D // TB):
            blk = stg[s, :, k * TB:(k + 1) * TB]
            if k % 2 == 0:
                t = blk.T
            else:
                t = dot_t(eye[...], blk).astype(BF16)
            wgu[m, k * TB:(k + 1) * TB, cols] = t

        @pl.when(j + NS < 2 * NTB)
        def _():
            gu_start(j + NS)

        @pl.when(j < lag)
        def _():
            relay(0, NC - lag + j)

        @pl.when((j >= 6) & (lax.rem(j, 2) == 0))
        def _():
            finish_own(0, (j - 6) // 2)

        @pl.when((j >= 9) & (lax.rem(j, 2) == 1))
        def _():
            finish_other(0, (j - 9) // 2)

    finish_other(0, NC - 1)

    _ph('norm1')
    norm(ga32)

    _ph('gate_up')
    def gate_up(start, width, keep):
        g = dot(xh[...], wgu[0, :, pl.ds(start, width)])
        u = dot(xh[...], wgu[1, :, pl.ds(start, width)])
        v = (g * jax.nn.sigmoid(g) * u).astype(BF16)
        act[:, pl.ds(start, keep)] = v[:, :keep]

    @pl.loop(0, FF // NT)
    def _(n):
        gate_up(pl.multiple_of(n * NT, NT), NT, NT)

        @pl.when(n < NC // 2)
        def _():
            down_copy(2 * n).start()
            down_copy(2 * n + 1).start()

    tail = FF // NT * NT
    gate_up(tail, FFP - tail, FF - tail)
    ssq[...] = jnp.zeros_like(ssq)

    _ph('down')
    lag2 = 2

    @pl.loop(0, NC)
    def _(c):
        down_copy(c).wait()
        put(1, c, dot(act[...], wgu[lax.rem(c, 2), :FFP, down_cols(c)]))

        @pl.when(c >= lag2)
        def _():
            relay(1, c - lag2)

    _ph('relay_tail')
    for cc in range(NC - lag2, NC):
        relay(1, cc)

    _ph('finish2')
    @pl.loop(0, NC)
    def _(c):
        finish_own(1, c)

        @pl.when(c > 0)
        def _():
            finish_other(1, c - 1)

    finish_other(1, NC - 1)
    _ph('norm2')
    norm(gm32)
    _ph('end')


def solution(mesh):
    tables = rope_tables()

    def local_layer(tokens, seq_lens, w_q, w_k, w_v, w_o, g_q, g_k, g_attn, g_mlp, w_gate, w_up, w_down):
        vmem = pl.BlockSpec(memory_space=pltpu.VMEM)
        anyspace = pl.BlockSpec(memory_space=pl.ANY)
        dma = pltpu.SemaphoreType.DMA
        y, kc, vc = pl.pallas_call(
            kernel,
            out_shape=(
                pltpu.VMEM((ROWS, D), BF16),
                pltpu.VMEM((PROMPTS, HEADS, SEQ, HEAD_DIM), BF16),
                pltpu.VMEM((PROMPTS, HEADS, SEQ, HEAD_DIM), BF16),
            ),
            in_specs=[pl.BlockSpec(memory_space=pltpu.SMEM)] + [anyspace] * 13,
            out_specs=(vmem,) * 3,
            scratch_shapes=[
                pltpu.VMEM((NS, TB, D), BF16),
                pltpu.VMEM((2, D, FFP), BF16),
                pltpu.VMEM((3, ROWS, QW), F32),
                pltpu.VMEM((ROWS, QW), BF16),
                pltpu.VMEM((NC, ROWS, CW), BF16),
                pltpu.VMEM((NC, HALF, CW), BF16),
                pltpu.VMEM((NC, HALF, CW), BF16),
                pltpu.VMEM((2, NC, HALF, CW), BF16),
                pltpu.VMEM((ROWS, D), BF16),
                pltpu.VMEM((ROWS, FFP), BF16),
                pltpu.VMEM((2, ROWS, HEAD_DIM), F32),
                pltpu.VMEM((QW // 128, 128), BF16),
                pltpu.VMEM((QW // 128, 128), BF16),
                pltpu.VMEM((D // 128, 128), BF16),
                pltpu.VMEM((D // 128, 128), BF16),
                pltpu.VMEM((D // 128, 128), F32),
                pltpu.VMEM((D // 128, 128), F32),
                pltpu.VMEM((8, 128), F32),
                pltpu.VMEM((3, 8, 128), F32),
                pltpu.VMEM((ROWS, 128), F32),
                pltpu.VMEM((TB, TB), BF16),
                pltpu.VMEM((HEADS, ROWS, HEAD_DIM), BF16),
                pltpu.VMEM((HEADS, ROWS, ROWS), BF16),
                dma((6,)), dma((16,)), dma((NS,)), dma((NC,)), dma((3,)), dma((3,)),
                dma((NC,)), dma((NC,)), dma((NC,)), dma((2, NC)), dma((NC,)), dma((NC,)),
            ],
            compiler_params=pltpu.CompilerParams(
                collective_id=0, has_side_effects=True, vmem_limit_bytes=VMEM_LIMIT),
            name="layer",
        )(seq_lens, tokens.reshape(ROWS, D), w_q, w_k, w_v, w_o,
          g_q.reshape(-1, 128), g_k.reshape(-1, 128), g_attn.reshape(-1, 128), g_mlp.reshape(-1, 128),
          w_gate.T, w_up.T, w_down, jnp.asarray(tables))
        return y.reshape(tokens.shape), kc, vc

    return jax.shard_map(local_layer, mesh=mesh, in_specs=(P('dp', None, None), P('dp'), P(None, 'tp'), P(None, 'tp'), P(None, 'tp'), P('tp', None), P('tp'), P('tp'), P(), P(), P(None, 'tp'), P(None, 'tp'), P('tp', None)), out_specs=(P('dp', None, None), P('dp', 'tp', None, None), P('dp', 'tp', None, None)), check_vma=False)
```

```python
import functools

import jax
import jax.numpy as jnp
import numpy as np
from jax import lax
from jax.experimental import pallas as pl
from jax.experimental.pallas import tpu as pltpu
from jax.sharding import PartitionSpec as P

HEAD_DIM = 128
ROPE_BASE = 500000.0
NORM_EPS = 1e-6

SEQ = 64
PROMPTS = 2
ROWS = SEQ * PROMPTS
HALF = ROWS // 2
D = 4096
QW = 1024
HEADS = QW // HEAD_DIM
FF = 2752
FFP = 2816
KC = 1024
CW = 512
NC = D // CW
TB = 256
NTB = FFP // TB
NS = 4
DEPTH = 4
NT = 512

VMEM_LIMIT = 60 * 2**20

F32 = jnp.float32
BF16 = jnp.bfloat16
MESH = pl.DeviceIdType.MESH


def rope_tables():
    half = HEAD_DIM // 2
    inv_freq = ROPE_BASE ** (-2.0 * np.arange(half, dtype=np.float64) / HEAD_DIM)
    inv_freq = inv_freq.astype(np.float32)
    angles = np.arange(SEQ, dtype=np.float32)[:, None] * inv_freq[None, :]
    cos = np.cos(angles.astype(np.float64)).astype(np.float32)
    sin = np.sin(angles.astype(np.float64)).astype(np.float32)
    cos2 = np.concatenate([cos, cos], axis=1)
    sin2 = np.concatenate([-sin, sin], axis=1)
    return np.stack([np.tile(cos2, (PROMPTS, 1)), np.tile(sin2, (PROMPTS, 1))])


def dot(a, b):
    return jnp.dot(a, b, preferred_element_type=F32)


def dot_t(a, b):
    return lax.dot_general(a, b, (((1,), (1,)), ((), ())), preferred_element_type=F32)


def row_scale(ssq):
    return lax.rsqrt(jnp.sum(ssq[...], axis=1, keepdims=True) * (1.0 / D) + NORM_EPS)


def add_norm(base, branch, rs, g32, c):
    for q in range(CW // 128):
        cols = pl.ds(pl.multiple_of(c * CW + q * 128, 128), 128)
        v = branch[:, cols].astype(F32) * rs * g32[pl.ds(c * (CW // 128) + q, 1), :]
        base[:, cols] = (base[:, cols].astype(F32) + v).astype(BF16)


_cur = []


def _ph(name):
    if _cur:
        _cur.pop().__exit__(None, None, None)
    if name != 'end':
        sc = jax.named_scope(name)
        sc.__enter__()
        _cur.append(sc)


def kernel(lens, tok, wq, wk, wv, wo, gq_h, gk_h, ga_h, gm_h, wg, wu, wd, tab_h,
           xh, full, ssq, gm32, kout, vout,
           stg, wgu, acc, ob, part, d2d, xsend, xrecv, act,
           tab, gq, gk, ga, gm, ga32, st, st_recv, eye, qb, pb,
           sem_in, sem_r, sem_g, sem_d, st_s, st_r,
           d_s, d_r, x_s, x_r, a_s, a_r):
    me = lax.axis_index("tp")
    core = lax.rem(me, 2)
    partner = me + 1 - 2 * core
    cross = lax.rem(me + 2, 4)
    mine = pl.ds(pl.multiple_of(core * HALF, HALF), HALF)
    theirs = pl.ds(pl.multiple_of((1 - core) * HALF, HALF), HALF)
    local = pltpu.make_async_copy

    small = [(tok, xh), (tab_h, tab), (gq_h, gq), (gk_h, gk), (ga_h, ga), (gm_h, gm)]

    def in_copy(i):
        return local(small[i][0], small[i][1], sem_in.at[i])

    def slot(i):
        i = i % 8
        return wgu.at[1, pl.ds((i % 4) * KC, KC), pl.ds((i // 4) * KC, KC)]

    qkv = [wq, wk, wv]

    def stream(i):
        if i < 12:
            src = qkv[i // 4].at[pl.ds((i % 4) * KC, KC), :]
        else:
            src = wo.at[:, pl.ds((i - 12) * KC, KC)]
        return local(src, slot(i), sem_r.at[i])

    def gu_copy(w, n, s):
        rows = TB if n < NTB - 1 else FF - TB * (NTB - 1)
        return local(w.at[pl.ds(n * TB, rows), :], stg.at[s, pl.ds(0, rows), :], sem_g.at[s])

    def gu_start(j):
        s = lax.rem(j, NS)
        n = lax.rem(j, NTB)
        for m, w in enumerate((wg, wu)):
            @pl.when((j // NTB == m) & (n < NTB - 1))
            def _():
                rows = pl.ds(pl.multiple_of(n * TB, TB), TB)
                local(w.at[rows, :], stg.at[s], sem_g.at[s]).start()

            @pl.when((j // NTB == m) & (n == NTB - 1))
            def _():
                gu_copy(w, NTB - 1, s).start()

    def gu_wait(j):
        s = lax.rem(j, NS)
        n = lax.rem(j, NTB)

        @pl.when(n < NTB - 1)
        def _():
            gu_copy(wg, 0, s).wait()

        @pl.when(n == NTB - 1)
        def _():
            gu_copy(wg, NTB - 1, s).wait()

    def down_cols(c):
        return pl.ds(pl.multiple_of(c // 2 * CW, CW), CW)

    def down_copy(c):
        return local(wd.at[:, pl.ds(pl.multiple_of(c * CW, CW), CW)],
                     wgu.at[lax.rem(c, 2), pl.ds(0, FF), down_cols(c)], sem_d.at[c])

    _ph('init')
    in_copy(0).start()
    stream(0).start()
    for i in range(1, 6):
        in_copy(i).start()
    for i in range(1, DEPTH):
        stream(i).start()

    barrier = pltpu.get_barrier_semaphore()
    for j in range(1, 4):
        pl.semaphore_signal(barrier, inc=1, device_id={"tp": lax.rem(me + j, 4)}, device_id_type=MESH)
    acc[...] = jnp.zeros_like(acc)
    st[...] = jnp.zeros_like(st)
    er = lax.broadcasted_iota(jnp.int32, (TB, TB), 0)
    ec = lax.broadcasted_iota(jnp.int32, (TB, TB), 1)
    eye[...] = (er == ec).astype(F32).astype(BF16)
    act[:, FF // 128 * 128:] = jnp.zeros((ROWS, FFP - FF // 128 * 128), BF16)
    _ph('wait_x')
    in_copy(0).wait()

    def qkv_step(i):
        stream(i).wait()
        w, k = i // 4, i % 4
        acc[w] += dot(xh[:, k * KC:(k + 1) * KC], slot(i)[...])
        if i + DEPTH < 16:
            stream(i + DEPTH).start()

    _ph('qk')
    for i in range(8):
        qkv_step(i)
    _ph('ssq_send')
    for w in range(2):
        t = jnp.zeros((ROWS, 128), F32)
        for h in range(HEADS):
            v = acc[w, :, h * 128:(h + 1) * 128]
            t = t + v * v
        st[w:w + 1, :] = jnp.sum(t.T, axis=0, keepdims=True)
    pl.semaphore_wait(barrier, 3)

    def st_copy(j):
        return pltpu.make_async_remote_copy(
            st, st_recv.at[j - 1], st_s.at[j - 1], st_r.at[j - 1],
            device_id={"tp": lax.rem(me + j, 4)}, device_id_type=MESH)

    for j in range(1, 4):
        st_copy(j).start()
    _ph('v')
    for i in range(8, 12):
        qkv_step(i)
    for j in range(NS):
        gu_copy(wg, j, j).start()
    _ph('vout')
    for i in range(1, 6):
        in_copy(i).wait()
    ga32[...] = ga[...].astype(F32)
    gm32[...] = gm[...].astype(F32)
    gq32, gk32 = gq[...].astype(F32), gk[...].astype(F32)
    for h in range(HEADS):
        vh = acc[2, :, h * 128:(h + 1) * 128].astype(BF16)
        vout[0, h] = vh[:SEQ]
        vout[1, h] = vh[SEQ:]
    _ph('st_wait')
    for j in range(1, 4):
        st_copy(j).wait()

    _ph('attn')
    tot = st[...] + st_recv[0] + st_recv[1] + st_recv[2]
    rs = lax.rsqrt(tot * (1.0 / D) + NORM_EPS)
    rq = jnp.broadcast_to(rs[0:1, :], (ROWS, 128)).T
    rk = jnp.broadcast_to(rs[1:2, :], (ROWS, 128)).T
    cos, sin = tab[0], tab[1]

    def rope(v):
        return v * cos + pltpu.roll(v, 64, axis=1) * sin

    ri = lax.broadcasted_iota(jnp.int32, (ROWS, ROWS), 0)
    ci = lax.broadcasted_iota(jnp.int32, (ROWS, ROWS), 1)
    same = (ri < SEQ) == (ci < SEQ)
    limit = jnp.where(ci < SEQ, lens[0], lens[1] + SEQ)
    allowed = same & (ci <= ri) & (ci < limit)
    for h in range(HEADS):
        cols = slice(h * 128, (h + 1) * 128)
        qb[h] = rope(acc[0, :, cols] * rq * gq32[h:h + 1]).astype(BF16)
        kh = rope(acc[1, :, cols] * rk * gk32[h:h + 1]).astype(BF16)
        kout[0, h] = kh[:SEQ]
        kout[1, h] = kh[SEQ:]
    for h in range(HEADS):
        kh = jnp.concatenate([kout[0, h], kout[1, h]], axis=0)
        s = jnp.where(allowed, dot_t(qb[h], kh) * HEAD_DIM ** -0.5, -1e30)
        e = jnp.exp(s - jnp.max(s, axis=1, keepdims=True))
        pb[h] = (e / jnp.sum(e, axis=1, keepdims=True)).astype(BF16)
    for h in range(HEADS):
        vh = jnp.concatenate([vout[0, h], vout[1, h]], axis=0)
        ob[:, h * 128:(h + 1) * 128] = dot(pb[h], vh).astype(BF16)

    def d_copy(ph, c):
        return pltpu.make_async_remote_copy(
            part.at[c, theirs, :], d2d.at[c], d_s.at[c], d_r.at[c],
            device_id={"tp": partner}, device_id_type=MESH)

    def x_copy(ph, c):
        return pltpu.make_async_remote_copy(
            xsend.at[c], xrecv.at[ph, c], x_s.at[c], x_r.at[ph, c],
            device_id={"tp": cross}, device_id_type=MESH)

    def cols_of(c):
        return pl.ds(pl.multiple_of(c * CW, CW), CW)

    def a_copy(ph, c):
        blk = full.at[mine, cols_of(c)]
        return pltpu.make_async_remote_copy(
            blk, blk, a_s.at[c], a_r.at[c],
            device_id={"tp": partner}, device_id_type=MESH)

    def put(ph, c, val):
        part[c] = val.astype(BF16)
        d_copy(ph, c).start()

    def relay(ph, c):
        d_copy(ph, c).wait()
        xsend[c] = (part[c, mine, :].astype(F32) + d2d[c].astype(F32)).astype(BF16)
        x_copy(ph, c).start()

    def add_sq(rows, c):
        v = full[rows, cols_of(c)].astype(F32)
        v = v * v
        t = v[:, 0:128]
        for q in range(1, CW // 128):
            t = t + v[:, q * 128:(q + 1) * 128]
        ssq[rows, :] += t

    def finish_own(ph, c):
        x_copy(ph, c).wait()
        s = xsend[c].astype(F32) + xrecv[ph, c].astype(F32)
        full[mine, cols_of(c)] = s.astype(BF16)
        a_copy(ph, c).start()
        add_sq(mine, c)

    def finish_other(ph, c):
        a_copy(ph, c).wait()
        add_sq(theirs, c)

    ssq[...] = jnp.zeros_like(ssq)
    lag = 2
    for c in range(4):
        stream(12 + c).wait()
        for half in range(2):
            cc = 2 * c + half
            put(0, cc, dot(ob[...], slot(12 + c)[:, half * CW:(half + 1) * CW]))
            if cc >= lag:
                relay(0, cc - lag)

    _ph('xpose')
    @pl.loop(0, 2 * NTB)
    def _(j):
        gu_wait(j)
        s, m, n = lax.rem(j, NS), j // NTB, lax.rem(j, NTB)
        cols = pl.ds(pl.multiple_of(n * TB, TB), TB)
        for k in range(D // TB):
            blk = stg[s, :, k * TB:(k + 1) * TB]
            if k % 2 == 0:
                t = blk.T
            else:
                t = dot_t(eye[...], blk).astype(BF16)
            wgu[m, k * TB:(k + 1) * TB, cols] = t

        @pl.when(j + NS < 2 * NTB)
        def _():
            gu_start(j + NS)

        @pl.when(j < lag)
        def _():
            relay(0, NC - lag + j)

        @pl.when((j >= 6) & (lax.rem(j, 2) == 0))
        def _():
            finish_own(0, (j - 6) // 2)

        @pl.when((j >= 9) & (lax.rem(j, 2) == 1))
        def _():
            finish_other(0, (j - 9) // 2)

    finish_other(0, NC - 1)

    _ph('norm1')
    rs1 = row_scale(ssq)

    @pl.loop(0, NC)
    def _(c):
        add_norm(xh, full, rs1, ga32, c)


    _ph('gate_up')
    def gate_up(start, width, keep):
        g = dot(xh[...], wgu[0, :, pl.ds(start, width)])
        u = dot(xh[...], wgu[1, :, pl.ds(start, width)])
        v = (g * jax.nn.sigmoid(g) * u).astype(BF16)
        act[:, pl.ds(start, keep)] = v[:, :keep]

    @pl.loop(0, FF // NT)
    def _(n):
        gate_up(pl.multiple_of(n * NT, NT), NT, NT)

        @pl.when(n < NC // 2)
        def _():
            down_copy(2 * n).start()
            down_copy(2 * n + 1).start()

    tail = FF // NT * NT
    gate_up(tail, FFP - tail, FF - tail)
    ssq[...] = jnp.zeros_like(ssq)

    _ph('down')
    lag2 = 2

    @pl.loop(0, NC)
    def _(c):
        down_copy(c).wait()
        put(1, c, dot(act[...], wgu[lax.rem(c, 2), :FFP, down_cols(c)]))

        @pl.when(c >= lag2)
        def _():
            relay(1, c - lag2)

    _ph('relay_tail')
    for cc in range(NC - lag2, NC):
        relay(1, cc)

    _ph('finish2')
    @pl.loop(0, NC)
    def _(c):
        finish_own(1, c)

        @pl.when(c > 0)
        def _():
            finish_other(1, c - 1)

    finish_other(1, NC - 1)
    _ph('end')


def store_kernel(h, m, ssq, g32, kc, vc, y_h, kc_h, vc_h, y, sem):
    kv = [pltpu.make_async_copy(a, b, sem.at[i]) for i, (a, b) in enumerate(((kc, kc_h), (vc, vc_h)))]
    for copy in kv:
        copy.start()
    rs = row_scale(ssq)
    blocks = []
    for c in range(NC):
        for q in range(CW // 128):
            cols = slice(c * CW + q * 128, c * CW + (q + 1) * 128)
            r = c * (CW // 128) + q
            v = m[:, cols].astype(F32) * rs * g32[r:r + 1, :]
            y[:, cols] = (h[:, cols].astype(F32) + v).astype(BF16)
        cols = pl.ds(c * CW, CW)
        blocks.append(pltpu.make_async_copy(y.at[:, cols], y_h.at[:, cols], sem.at[2 + c]))
        blocks[-1].start()
    for copy in kv + blocks:
        copy.wait()


def solution(mesh):
    tables = rope_tables()

    def local_layer(tokens, seq_lens, w_q, w_k, w_v, w_o, g_q, g_k, g_attn, g_mlp, w_gate, w_up, w_down):
        vmem = pl.BlockSpec(memory_space=pltpu.VMEM)
        anyspace = pl.BlockSpec(memory_space=pl.ANY)
        dma = pltpu.SemaphoreType.DMA
        outs = pl.pallas_call(
            kernel,
            out_shape=(
                pltpu.VMEM((ROWS, D), BF16),
                pltpu.VMEM((ROWS, D), BF16),
                pltpu.VMEM((ROWS, 128), F32),
                pltpu.VMEM((D // 128, 128), F32),
                pltpu.VMEM((PROMPTS, HEADS, SEQ, HEAD_DIM), BF16),
                pltpu.VMEM((PROMPTS, HEADS, SEQ, HEAD_DIM), BF16),
            ),
            in_specs=[pl.BlockSpec(memory_space=pltpu.SMEM)] + [anyspace] * 13,
            out_specs=(vmem,) * 6,
            scratch_shapes=[
                pltpu.VMEM((NS, TB, D), BF16),
                pltpu.VMEM((2, D, FFP), BF16),
                pltpu.VMEM((3, ROWS, QW), F32),
                pltpu.VMEM((ROWS, QW), BF16),
                pltpu.VMEM((NC, ROWS, CW), BF16),
                pltpu.VMEM((NC, HALF, CW), BF16),
                pltpu.VMEM((NC, HALF, CW), BF16),
                pltpu.VMEM((2, NC, HALF, CW), BF16),
                pltpu.VMEM((ROWS, FFP), BF16),
                pltpu.VMEM((2, ROWS, HEAD_DIM), F32),
                pltpu.VMEM((QW // 128, 128), BF16),
                pltpu.VMEM((QW // 128, 128), BF16),
                pltpu.VMEM((D // 128, 128), BF16),
                pltpu.VMEM((D // 128, 128), BF16),
                pltpu.VMEM((D // 128, 128), F32),
                pltpu.VMEM((8, 128), F32),
                pltpu.VMEM((3, 8, 128), F32),
                pltpu.VMEM((TB, TB), BF16),
                pltpu.VMEM((HEADS, ROWS, HEAD_DIM), BF16),
                pltpu.VMEM((HEADS, ROWS, ROWS), BF16),
                dma((6,)), dma((16,)), dma((NS,)), dma((NC,)), dma((3,)), dma((3,)),
                dma((NC,)), dma((NC,)), dma((NC,)), dma((2, NC)), dma((NC,)), dma((NC,)),
            ],
            compiler_params=pltpu.CompilerParams(
                collective_id=0, has_side_effects=True, vmem_limit_bytes=VMEM_LIMIT),
            name="layer",
        )(seq_lens, tokens.reshape(ROWS, D), w_q, w_k, w_v, w_o,
          g_q.reshape(-1, 128), g_k.reshape(-1, 128), g_attn.reshape(-1, 128), g_mlp.reshape(-1, 128),
          w_gate.T, w_up.T, w_down, jnp.asarray(tables))
        outs = [pltpu.with_memory_space_constraint(o, pltpu.VMEM) for o in outs]
        y, kc, vc = pl.pallas_call(
            store_kernel,
            out_shape=(
                jax.ShapeDtypeStruct((ROWS, D), BF16),
                jax.ShapeDtypeStruct((PROMPTS, HEADS, SEQ, HEAD_DIM), BF16),
                jax.ShapeDtypeStruct((PROMPTS, HEADS, SEQ, HEAD_DIM), BF16),
            ),
            in_specs=[vmem] * 6,
            out_specs=(anyspace,) * 3,
            scratch_shapes=[pltpu.VMEM((ROWS, D), BF16), dma((2 + NC,))],
            compiler_params=pltpu.CompilerParams(vmem_limit_bytes=3 * 2**19),
            name="store",
        )(*outs)
        return y.reshape(tokens.shape), kc, vc

    return jax.shard_map(local_layer, mesh=mesh, in_specs=(P('dp', None, None), P('dp'), P(None, 'tp'), P(None, 'tp'), P(None, 'tp'), P('tp', None), P('tp'), P('tp'), P(), P(), P(None, 'tp'), P(None, 'tp'), P('tp', None)), out_specs=(P('dp', None, None), P('dp', 'tp', None, None), P('dp', 'tp', None, None)), check_vma=False)
```

```python
import functools

import jax
import jax.numpy as jnp
import numpy as np
from jax import lax
from jax.experimental import pallas as pl
from jax.experimental.pallas import tpu as pltpu
from jax.sharding import PartitionSpec as P

HEAD_DIM = 128
ROPE_BASE = 500000.0
NORM_EPS = 1e-6

SEQ = 64
PROMPTS = 2
ROWS = SEQ * PROMPTS
HALF = ROWS // 2
D = 4096
QW = 1024
HEADS = QW // HEAD_DIM
FF = 2752
FFP = 2816
FFW = FFP + 128
DW = D + 128
KC = 1024
CW = 512
NC = D // CW
TB = 256
NTB = FFP // TB
NS = 4
DEPTH = 4
NT = 512

VMEM_LIMIT = 61 * 2**20

F32 = jnp.float32
BF16 = jnp.bfloat16
MESH = pl.DeviceIdType.MESH


def rope_tables():
    half = HEAD_DIM // 2
    inv_freq = ROPE_BASE ** (-2.0 * np.arange(half, dtype=np.float64) / HEAD_DIM)
    inv_freq = inv_freq.astype(np.float32)
    angles = np.arange(SEQ, dtype=np.float32)[:, None] * inv_freq[None, :]
    cos = np.cos(angles.astype(np.float64)).astype(np.float32)
    sin = np.sin(angles.astype(np.float64)).astype(np.float32)
    cos2 = np.concatenate([cos, cos], axis=1)
    sin2 = np.concatenate([-sin, sin], axis=1)
    return np.stack([np.tile(cos2, (PROMPTS, 1)), np.tile(sin2, (PROMPTS, 1))])


def dot(a, b):
    return jnp.dot(a, b, preferred_element_type=F32)


def dot_t(a, b):
    return lax.dot_general(a, b, (((1,), (1,)), ((), ())), preferred_element_type=F32)


def row_scale(ssq):
    return lax.rsqrt(jnp.sum(ssq[...], axis=1, keepdims=True) * (1.0 / D) + NORM_EPS)


def add_norm(base, branch, rs, g32, c):
    for q in range(CW // 128):
        col = c * CW + q * 128
        cols = pl.ds(col if isinstance(c, int) else pl.multiple_of(col, 128), 128)
        v = branch[:, cols].astype(F32) * rs * g32[pl.ds(c * (CW // 128) + q, 1), :]
        base[:, cols] = (base[:, cols].astype(F32) + v).astype(BF16)


_cur = []


def _ph(name):
    if _cur:
        _cur.pop().__exit__(None, None, None)
    if name != 'end':
        sc = jax.named_scope(name)
        sc.__enter__()
        _cur.append(sc)


def kernel(lens, tok, wq, wk, wv, wo, gq_h, gk_h, ga_h, gm_h, wg, wu, wd, tab_h,
           xh, full, ssq, gm32, kout, vout,
           stg, wgu, acc, ob, part, d2d, xsend, xrecv, act,
           tab, gq, gk, ga, gm, ga32, st, st_recv, eye,
           sem_w, st_s, st_r,
           d_s, d_r, x_s, x_r, a_s, a_r):
    me = lax.axis_index("tp")
    core = lax.rem(me, 2)
    partner = me + 1 - 2 * core
    cross = lax.rem(me + 2, 4)
    mine = pl.ds(pl.multiple_of(core * HALF, HALF), HALF)
    theirs = pl.ds(pl.multiple_of((1 - core) * HALF, HALF), HALF)
    local = pltpu.make_async_copy

    small = [(tok, xh.at[:, pl.ds(0, D)]), (tab_h, tab), (gq_h, gq), (gk_h, gk), (ga_h, ga), (gm_h, gm)]

    def in_copy(i):
        return local(small[i][0], small[i][1], sem_w.at[4 + i])

    def slot(i):
        i = i % 8
        return wgu.at[1, pl.ds((i % 4) * KC, KC), pl.ds((i // 4) * KC, KC)]

    qkv = [wq, wk, wv]

    def stream(i):
        if i < 12:
            src = qkv[i // 4].at[pl.ds((i % 4) * KC, KC), :]
        else:
            src = wo.at[:, pl.ds((i - 12) * KC, KC)]
        return local(src, slot(i), sem_w.at[i % DEPTH])

    def gu_copy(w, n, s):
        rows = TB if n < NTB - 1 else FF - TB * (NTB - 1)
        return local(w.at[pl.ds(n * TB, rows), :], stg.at[s, pl.ds(0, rows), :], sem_w.at[4 + s])

    def gu_start(j):
        s = lax.rem(j, NS)
        n = lax.rem(j, NTB)
        for m, w in enumerate((wg, wu)):
            @pl.when((j // NTB == m) & (n < NTB - 1))
            def _():
                rows = pl.ds(pl.multiple_of(n * TB, TB), TB)
                local(w.at[rows, :], stg.at[s], sem_w.at[4 + s]).start()

            @pl.when((j // NTB == m) & (n == NTB - 1))
            def _():
                gu_copy(w, NTB - 1, s).start()

    def gu_wait(j):
        s = lax.rem(j, NS)
        n = lax.rem(j, NTB)

        @pl.when(n < NTB - 1)
        def _():
            gu_copy(wg, 0, s).wait()

        @pl.when(n == NTB - 1)
        def _():
            gu_copy(wg, NTB - 1, s).wait()

    def down_cols(c):
        return pl.ds(pl.multiple_of(c // 2 * CW, CW), CW)

    def down_copy(c):
        return local(wd.at[:, pl.ds(pl.multiple_of(c * CW, CW), CW)],
                     wgu.at[lax.rem(c, 2), pl.ds(0, FF), down_cols(c)], sem_w.at[c])

    _ph('init')
    in_copy(0).start()
    stream(0).start()
    for i in range(1, 6):
        in_copy(i).start()
    for i in range(1, DEPTH):
        stream(i).start()

    barrier = pltpu.get_barrier_semaphore()
    for j in range(1, 4):
        pl.semaphore_signal(barrier, inc=1, device_id={"tp": lax.rem(me + j, 4)}, device_id_type=MESH)
    acc[...] = jnp.zeros_like(acc)
    st[...] = jnp.zeros_like(st)
    er = lax.broadcasted_iota(jnp.int32, (TB, TB), 0)
    ec = lax.broadcasted_iota(jnp.int32, (TB, TB), 1)
    eye[...] = (er == ec).astype(F32).astype(BF16)
    act[:, FF // 128 * 128:] = jnp.zeros((ROWS, FFP - FF // 128 * 128), BF16)
    _ph('wait_x')
    in_copy(0).wait()

    def qkv_step(i):
        stream(i).wait()
        w, k = i // 4, i % 4
        acc[w] += dot(xh[:, k * KC:(k + 1) * KC], slot(i)[...])
        if i + DEPTH < 16:
            stream(i + DEPTH).start()

    _ph('qk')
    for i in range(8):
        qkv_step(i)
    _ph('ssq_send')
    for w in range(2):
        t = jnp.zeros((ROWS, 128), F32)
        for h in range(HEADS):
            v = acc[w, :, h * 128:(h + 1) * 128]
            t = t + v * v
        st[w:w + 1, :] = jnp.sum(t.T, axis=0, keepdims=True)
    pl.semaphore_wait(barrier, 3)

    def st_copy(j):
        return pltpu.make_async_remote_copy(
            st, st_recv.at[j - 1], st_s.at[j - 1], st_r.at[j - 1],
            device_id={"tp": lax.rem(me + j, 4)}, device_id_type=MESH)

    for j in range(1, 4):
        st_copy(j).start()
    _ph('v')
    for i in range(8, 12):
        qkv_step(i)
    for i in range(1, 6):
        in_copy(i).wait()
    for j in range(NS):
        gu_copy(wg, j, j).start()
    _ph('vout')
    ga32[...] = ga[...].astype(F32)
    gm32[...] = gm[...].astype(F32)
    gq32, gk32 = gq[...].astype(F32), gk[...].astype(F32)
    for h in range(HEADS):
        vh = acc[2, :, h * 128:(h + 1) * 128].astype(BF16)
        vout[0, h] = vh[:SEQ]
        vout[1, h] = vh[SEQ:]
    _ph('st_wait')
    for j in range(1, 4):
        st_copy(j).wait()

    _ph('attn')
    tot = st[...] + st_recv[0] + st_recv[1] + st_recv[2]
    rs = lax.rsqrt(tot * (1.0 / D) + NORM_EPS)
    rq = jnp.broadcast_to(rs[0:1, :], (ROWS, 128)).T
    rk = jnp.broadcast_to(rs[1:2, :], (ROWS, 128)).T
    cos, sin = tab[0], tab[1]

    def rope(v):
        return v * cos + pltpu.roll(v, 64, axis=1) * sin

    ri = lax.broadcasted_iota(jnp.int32, (ROWS, ROWS), 0)
    ci = lax.broadcasted_iota(jnp.int32, (ROWS, ROWS), 1)
    same = (ri < SEQ) == (ci < SEQ)
    limit = jnp.where(ci < SEQ, lens[0], lens[1] + SEQ)
    allowed = same & (ci <= ri) & (ci < limit)
    for h in range(HEADS):
        cols = slice(h * 128, (h + 1) * 128)
        part[h // 4, :, h % 4 * 128:(h % 4 + 1) * 128] = rope(acc[0, :, cols] * rq * gq32[h:h + 1]).astype(BF16)
        kh = rope(acc[1, :, cols] * rk * gk32[h:h + 1]).astype(BF16)
        kout[0, h] = kh[:SEQ]
        kout[1, h] = kh[SEQ:]
    for h in range(HEADS):
        kh = jnp.concatenate([kout[0, h], kout[1, h]], axis=0)
        s = jnp.where(allowed, dot_t(part[h // 4, :, h % 4 * 128:(h % 4 + 1) * 128], kh) * HEAD_DIM ** -0.5, -1e30)
        e = jnp.exp(s - jnp.max(s, axis=1, keepdims=True))
        part[2 + h // 4, :, h % 4 * 128:(h % 4 + 1) * 128] = (e / jnp.sum(e, axis=1, keepdims=True)).astype(BF16)
    for h in range(HEADS):
        vh = jnp.concatenate([vout[0, h], vout[1, h]], axis=0)
        ob[:, h * 128:(h + 1) * 128] = dot(part[2 + h // 4, :, h % 4 * 128:(h % 4 + 1) * 128], vh).astype(BF16)

    def d_copy(ph, c):
        return pltpu.make_async_remote_copy(
            part.at[c, theirs, :], d2d.at[c], d_s.at[lax.rem(c, 4)], d_r.at[c],
            device_id={"tp": partner}, device_id_type=MESH)

    def x_copy(ph, c):
        return pltpu.make_async_remote_copy(
            xsend.at[c], xrecv.at[ph, c], x_s.at[c], x_r.at[ph, c],
            device_id={"tp": cross}, device_id_type=MESH)

    def cols_of(c):
        return pl.ds(pl.multiple_of(c * CW, CW), CW)

    def a_copy(ph, c):
        blk = full.at[mine, cols_of(c)]
        return pltpu.make_async_remote_copy(
            blk, blk, a_s.at[lax.rem(c, 4)], a_r.at[c],
            device_id={"tp": partner}, device_id_type=MESH)

    def put(ph, c, val):
        part[c] = val.astype(BF16)
        d_copy(ph, c).start()

    def relay(ph, c):
        d_copy(ph, c).wait()
        xsend[c] = (part[c, mine, :].astype(F32) + d2d[c].astype(F32)).astype(BF16)
        x_copy(ph, c).start()

    def add_sq(rows, c):
        v = full[rows, cols_of(c)].astype(F32)
        v = v * v
        t = v[:, 0:128]
        for q in range(1, CW // 128):
            t = t + v[:, q * 128:(q + 1) * 128]
        ssq[rows, :] += t

    def finish_own(ph, c):
        x_copy(ph, c).wait()
        s = xsend[c].astype(F32) + xrecv[ph, c].astype(F32)
        full[mine, cols_of(c)] = s.astype(BF16)
        a_copy(ph, c).start()
        add_sq(mine, c)

    def finish_other(ph, c):
        a_copy(ph, c).wait()
        add_sq(theirs, c)

    ssq[...] = jnp.zeros_like(ssq)
    lag = 2
    for c in range(4):
        stream(12 + c).wait()
        for half in range(2):
            cc = 2 * c + half
            put(0, cc, dot(ob[...], slot(12 + c)[:, half * CW:(half + 1) * CW]))
            if cc >= lag:
                relay(0, cc - lag)

    _ph('xpose')
    @pl.loop(0, 2 * NTB)
    def _(j):
        gu_wait(j)
        s, m, n = lax.rem(j, NS), j // NTB, lax.rem(j, NTB)
        cols = pl.ds(pl.multiple_of(n * TB, TB), TB)
        for k in range(D // TB):
            blk = stg[s, :, k * TB:(k + 1) * TB]
            if k % 2 == 0:
                t = blk.T
            else:
                t = dot_t(eye[...], blk).astype(BF16)
            wgu[m, k * TB:(k + 1) * TB, cols] = t

        @pl.when(j + NS < 2 * NTB)
        def _():
            gu_start(j + NS)

        @pl.when(j < lag)
        def _():
            relay(0, NC - lag + j)

        @pl.when((j >= 6) & (lax.rem(j, 2) == 0))
        def _():
            finish_own(0, (j - 6) // 2)

        @pl.when((j >= 9) & (lax.rem(j, 2) == 1))
        def _():
            finish_other(0, (j - 9) // 2)

    finish_other(0, NC - 1)

    _ph('norm1')
    rs1 = row_scale(ssq)

    for c in range(NC):
        add_norm(xh, full, rs1, ga32, c)


    def gate_up(start, width, keep):
        g = dot(xh[:, :D], wgu[0, :, pl.ds(start, width)])
        u = dot(xh[:, :D], wgu[1, :, pl.ds(start, width)])
        v = (g * jax.nn.sigmoid(g) * u).astype(BF16)
        act[:, pl.ds(start, keep)] = v[:, :keep]

    gate_up(0, NT, NT)
    down_copy(0).start()
    down_copy(1).start()

    @pl.loop(1, FF // NT)
    def _(n):
        gate_up(pl.multiple_of(n * NT, NT), NT, NT)

        @pl.when(n < NC // 2)
        def _():
            down_copy(2 * n).start()
            down_copy(2 * n + 1).start()

    tail = FF // NT * NT
    gate_up(tail, FFP - tail, FF - tail)
    ssq[...] = jnp.zeros_like(ssq)

    _ph('down')
    lag2 = 2

    @pl.loop(0, NC)
    def _(c):
        down_copy(c).wait()
        put(1, c, dot(act[...], wgu[lax.rem(c, 2), :FFP, down_cols(c)]))

        @pl.when(c >= lag2)
        def _():
            relay(1, c - lag2)

    _ph('relay_tail')
    for cc in range(NC - lag2, NC):
        relay(1, cc)

    _ph('finish2')
    @pl.loop(0, NC)
    def _(c):
        finish_own(1, c)

        @pl.when(c > 0)
        def _():
            finish_other(1, c - 1)

    finish_other(1, NC - 1)
    _ph('end')


def store_kernel(h, m, ssq, g32, kc, vc, y_h, kc_h, vc_h, y, sem):
    kv = [pltpu.make_async_copy(a, b, sem.at[i]) for i, (a, b) in enumerate(((kc, kc_h), (vc, vc_h)))]
    for copy in kv:
        copy.start()
    rs = row_scale(ssq)
    blocks = []
    for c in range(NC):
        for q in range(CW // 128):
            cols = slice(c * CW + q * 128, c * CW + (q + 1) * 128)
            r = c * (CW // 128) + q
            v = m[:, cols].astype(F32) * rs * g32[r:r + 1, :]
            y[:, cols] = (h[:, cols].astype(F32) + v).astype(BF16)
        cols = pl.ds(c * CW, CW)
        blocks.append(pltpu.make_async_copy(y.at[:, cols], y_h.at[:, cols], sem.at[2 + c]))
        blocks[-1].start()
    for copy in kv + blocks:
        copy.wait()


def solution(mesh):
    tables = rope_tables()

    def local_layer(tokens, seq_lens, w_q, w_k, w_v, w_o, g_q, g_k, g_attn, g_mlp, w_gate, w_up, w_down):
        vmem = pl.BlockSpec(memory_space=pltpu.VMEM)
        anyspace = pl.BlockSpec(memory_space=pl.ANY)
        dma = pltpu.SemaphoreType.DMA
        outs = pl.pallas_call(
            kernel,
            out_shape=(
                pltpu.VMEM((ROWS, DW), BF16),
                pltpu.VMEM((ROWS, D), BF16),
                pltpu.VMEM((ROWS, 128), F32),
                pltpu.VMEM((D // 128, 128), F32),
                pltpu.VMEM((PROMPTS, HEADS, SEQ, HEAD_DIM), BF16),
                pltpu.VMEM((PROMPTS, HEADS, SEQ, HEAD_DIM), BF16),
            ),
            in_specs=[pl.BlockSpec(memory_space=pltpu.SMEM)] + [anyspace] * 13,
            out_specs=(vmem,) * 6,
            scratch_shapes=[
                pltpu.VMEM((NS, TB, D), BF16),
                pltpu.VMEM((2, D, FFW), BF16),
                pltpu.VMEM((3, ROWS, QW), F32),
                pltpu.VMEM((ROWS, QW), BF16),
                pltpu.VMEM((NC, ROWS, CW), BF16),
                pltpu.VMEM((NC, HALF, CW), BF16),
                pltpu.VMEM((NC, HALF, CW), BF16),
                pltpu.VMEM((2, NC, HALF, CW), BF16),
                pltpu.VMEM((ROWS, FFP), BF16),
                pltpu.VMEM((2, ROWS, HEAD_DIM), F32),
                pltpu.VMEM((QW // 128, 128), BF16),
                pltpu.VMEM((QW // 128, 128), BF16),
                pltpu.VMEM((D // 128, 128), BF16),
                pltpu.VMEM((D // 128, 128), BF16),
                pltpu.VMEM((D // 128, 128), F32),
                pltpu.VMEM((8, 128), F32),
                pltpu.VMEM((3, 8, 128), F32),
                pltpu.VMEM((TB, TB), BF16),
                dma((10,)), dma((3,)), dma((3,)),
                dma((4,)), dma((NC,)), dma((NC,)), dma((2, NC)), dma((4,)), dma((NC,)),
            ],
            compiler_params=pltpu.CompilerParams(
                collective_id=0, has_side_effects=True, vmem_limit_bytes=VMEM_LIMIT),
            name="layer",
        )(seq_lens, tokens.reshape(ROWS, D), w_q, w_k, w_v, w_o,
          g_q.reshape(-1, 128), g_k.reshape(-1, 128), g_attn.reshape(-1, 128), g_mlp.reshape(-1, 128),
          w_gate.T, w_up.T, w_down, jnp.asarray(tables))
        outs = [pltpu.with_memory_space_constraint(o, pltpu.VMEM) for o in outs]
        y, kc, vc = pl.pallas_call(
            store_kernel,
            out_shape=(
                jax.ShapeDtypeStruct((ROWS, D), BF16),
                jax.ShapeDtypeStruct((PROMPTS, HEADS, SEQ, HEAD_DIM), BF16),
                jax.ShapeDtypeStruct((PROMPTS, HEADS, SEQ, HEAD_DIM), BF16),
            ),
            in_specs=[vmem] * 6,
            out_specs=(anyspace,) * 3,
            scratch_shapes=[pltpu.VMEM((ROWS, D), BF16), dma((2 + NC,))],
            compiler_params=pltpu.CompilerParams(vmem_limit_bytes=3 * 2**19),
            name="store",
        )(*outs)
        return y.reshape(tokens.shape), kc, vc

    return jax.shard_map(local_layer, mesh=mesh, in_specs=(P('dp', None, None), P('dp'), P(None, 'tp'), P(None, 'tp'), P(None, 'tp'), P('tp', None), P('tp'), P('tp'), P(), P(), P(None, 'tp'), P(None, 'tp'), P('tp', None)), out_specs=(P('dp', None, None), P('dp', 'tp', None, None), P('dp', 'tp', None, None)), check_vma=False)
```

```python
import functools

import jax
import jax.numpy as jnp
import numpy as np
from jax import lax
from jax.experimental import pallas as pl
from jax.experimental.pallas import tpu as pltpu
from jax.sharding import PartitionSpec as P

HEAD_DIM = 128
ROPE_BASE = 500000.0
NORM_EPS = 1e-6

SEQ = 64
PROMPTS = 2
ROWS = SEQ * PROMPTS
HALF = ROWS // 2
D = 4096
QW = 1024
HEADS = QW // HEAD_DIM
FF = 2752
FFP = 2816
FFW = FFP + 128
DW = D + 128
KC = 1024
CW = 512
NC = D // CW
TB = 256
NTB = FFP // TB
NS = 4
DEPTH = 4
NEXT = {i: (i + 4,) for i in range(8)}
NEXT.update({9: (12,), 10: (13,), 11: (14, 15)})
NT = 512

VMEM_LIMIT = 61 * 2**20

F32 = jnp.float32
BF16 = jnp.bfloat16
MESH = pl.DeviceIdType.MESH


def rope_tables():
    half = HEAD_DIM // 2
    inv_freq = ROPE_BASE ** (-2.0 * np.arange(half, dtype=np.float64) / HEAD_DIM)
    inv_freq = inv_freq.astype(np.float32)
    angles = np.arange(SEQ, dtype=np.float32)[:, None] * inv_freq[None, :]
    cos = np.cos(angles.astype(np.float64)).astype(np.float32)
    sin = np.sin(angles.astype(np.float64)).astype(np.float32)
    cos2 = np.concatenate([cos, cos], axis=1)
    sin2 = np.concatenate([-sin, sin], axis=1)
    return np.stack([np.tile(cos2, (PROMPTS, 1)), np.tile(sin2, (PROMPTS, 1))])


def dot(a, b):
    return jnp.dot(a, b, preferred_element_type=F32)


def dot_t(a, b):
    return lax.dot_general(a, b, (((1,), (1,)), ((), ())), preferred_element_type=F32)


def row_scale(ssq):
    return lax.rsqrt(jnp.sum(ssq[...], axis=1, keepdims=True) * (1.0 / D) + NORM_EPS)


def add_norm(base, branch, rs, g32, c):
    for q in range(CW // 128):
        col = c * CW + q * 128
        cols = pl.ds(col if isinstance(c, int) else pl.multiple_of(col, 128), 128)
        v = branch[:, cols].astype(F32) * rs * g32[pl.ds(c * (CW // 128) + q, 1), :]
        base[:, cols] = (base[:, cols].astype(F32) + v).astype(BF16)


_cur = []


def _ph(name):
    if _cur:
        _cur.pop().__exit__(None, None, None)
    if name != 'end':
        sc = jax.named_scope(name)
        sc.__enter__()
        _cur.append(sc)


def kernel(lens_h, tok, wq, wk, wv, wo, gq_h, gk_h, ga_h, gm_h, wg, wu, wd, tab_h,
           xh, full, ssq, gm32, kout, vout,
           stg, wgu, acc, ob, part, d2d, xsend, xrecv, act,
           tab, gq, gk, ga, gm, ga32, st, st_recv, eye, lens,
           sem_w, st_s, st_r,
           d_s, d_r, x_s, x_r, a_s, a_r):
    me = lax.axis_index("tp")
    core = lax.rem(me, 2)
    partner = me + 1 - 2 * core
    cross = lax.rem(me + 2, 4)
    mine = pl.ds(pl.multiple_of(core * HALF, HALF), HALF)
    theirs = pl.ds(pl.multiple_of((1 - core) * HALF, HALF), HALF)
    local = pltpu.make_async_copy

    small = [(tok, xh.at[:, pl.ds(0, D)]), (tab_h, tab), (gq_h, gq), (gk_h, gk), (ga_h, ga), (gm_h, gm), (lens_h, lens)]

    def in_copy(i):
        return local(small[i][0], small[i][1], sem_w.at[4 + i])

    def slot(i):
        i = i % 8
        return wgu.at[1, pl.ds((i % 4) * KC, KC), pl.ds((i // 4) * KC, KC)]

    qkv = [wq, wk, wv]

    def stream(i):
        if i < 12:
            src = qkv[i // 4].at[pl.ds((i % 4) * KC, KC), :]
        else:
            src = wo.at[:, pl.ds((i - 12) * KC, KC)]
        return local(src, slot(i), sem_w.at[i % DEPTH])

    def gu_copy(w, n, s):
        rows = TB if n < NTB - 1 else FF - TB * (NTB - 1)
        return local(w.at[pl.ds(n * TB, rows), :], stg.at[s, pl.ds(0, rows), :], sem_w.at[4 + s])

    def gu_start(j):
        s = lax.rem(j, NS)
        n = lax.rem(j, NTB)
        for m, w in enumerate((wg, wu)):
            @pl.when((j // NTB == m) & (n < NTB - 1))
            def _():
                rows = pl.ds(pl.multiple_of(n * TB, TB), TB)
                local(w.at[rows, :], stg.at[s], sem_w.at[4 + s]).start()

            @pl.when((j // NTB == m) & (n == NTB - 1))
            def _():
                gu_copy(w, NTB - 1, s).start()

    def gu_wait(j):
        s = lax.rem(j, NS)
        n = lax.rem(j, NTB)

        @pl.when(n < NTB - 1)
        def _():
            gu_copy(wg, 0, s).wait()

        @pl.when(n == NTB - 1)
        def _():
            gu_copy(wg, NTB - 1, s).wait()

    def down_cols(c):
        return pl.ds(pl.multiple_of(c // 2 * CW, CW), CW)

    def down_copy(c):
        return local(wd.at[:, pl.ds(pl.multiple_of(c * CW, CW), CW)],
                     wgu.at[lax.rem(c, 2), pl.ds(0, FF), down_cols(c)], sem_w.at[c])

    _ph('init')
    in_copy(0).start()
    stream(0).start()
    for i in range(1, 7):
        in_copy(i).start()
    for i in range(1, DEPTH):
        stream(i).start()

    barrier = pltpu.get_barrier_semaphore()
    for j in range(1, 4):
        pl.semaphore_signal(barrier, inc=1, device_id={"tp": lax.rem(me + j, 4)}, device_id_type=MESH)
    acc[...] = jnp.zeros_like(acc)
    st[...] = jnp.zeros_like(st)
    er = lax.broadcasted_iota(jnp.int32, (TB, TB), 0)
    ec = lax.broadcasted_iota(jnp.int32, (TB, TB), 1)
    eye[...] = (er == ec).astype(F32).astype(BF16)
    act[:, FF // 128 * 128:] = jnp.zeros((ROWS, FFP - FF // 128 * 128), BF16)
    _ph('wait_x')
    in_copy(0).wait()

    def qkv_step(i):
        stream(i).wait()
        w, k = i // 4, i % 4
        acc[w] += dot(xh[:, k * KC:(k + 1) * KC], slot(i)[...])
        for n in NEXT.get(i, ()):
            stream(n).start()

    _ph('qk')
    for i in range(8):
        qkv_step(i)
    _ph('ssq_send')
    for w in range(2):
        t = jnp.zeros((ROWS, 128), F32)
        for h in range(HEADS):
            v = acc[w, :, h * 128:(h + 1) * 128]
            t = t + v * v
        st[w:w + 1, :] = jnp.sum(t.T, axis=0, keepdims=True)
    pl.semaphore_wait(barrier, 3)

    def st_copy(j):
        return pltpu.make_async_remote_copy(
            st, st_recv.at[j - 1], st_s.at[j - 1], st_r.at[j - 1],
            device_id={"tp": lax.rem(me + j, 4)}, device_id_type=MESH)

    for j in range(1, 4):
        st_copy(j).start()
    _ph('v')
    for i in range(8, 12):
        qkv_step(i)
    for i in range(1, 7):
        in_copy(i).wait()
    for j in range(NS):
        gu_copy(wg, j, j).start()
    _ph('vout')
    ga32[...] = ga[...].astype(F32)
    gm32[...] = gm[...].astype(F32)
    gq32, gk32 = gq[...].astype(F32), gk[...].astype(F32)
    for h in range(HEADS):
        vh = acc[2, :, h * 128:(h + 1) * 128].astype(BF16)
        vout[0, h] = vh[:SEQ]
        vout[1, h] = vh[SEQ:]
    _ph('st_wait')
    for j in range(1, 4):
        st_copy(j).wait()

    _ph('attn')
    tot = st[...] + st_recv[0] + st_recv[1] + st_recv[2]
    rs = lax.rsqrt(tot * (1.0 / D) + NORM_EPS)
    rq = jnp.broadcast_to(rs[0:1, :], (ROWS, 128)).T
    rk = jnp.broadcast_to(rs[1:2, :], (ROWS, 128)).T
    cos, sin = tab[0], tab[1]

    def rope(v):
        return v * cos + pltpu.roll(v, 64, axis=1) * sin

    ri = lax.broadcasted_iota(jnp.int32, (ROWS, ROWS), 0)
    ci = lax.broadcasted_iota(jnp.int32, (ROWS, ROWS), 1)
    same = (ri < SEQ) == (ci < SEQ)
    limit = jnp.where(ci < SEQ, lens[0], lens[1] + SEQ)
    allowed = same & (ci <= ri) & (ci < limit)
    for h in range(HEADS):
        cols = slice(h * 128, (h + 1) * 128)
        part[h // 4, :, h % 4 * 128:(h % 4 + 1) * 128] = rope(acc[0, :, cols] * rq * gq32[h:h + 1]).astype(BF16)
        kh = rope(acc[1, :, cols] * rk * gk32[h:h + 1]).astype(BF16)
        kout[0, h] = kh[:SEQ]
        kout[1, h] = kh[SEQ:]
    for h in range(HEADS):
        kh = jnp.concatenate([kout[0, h], kout[1, h]], axis=0)
        s = jnp.where(allowed, dot_t(part[h // 4, :, h % 4 * 128:(h % 4 + 1) * 128], kh) * HEAD_DIM ** -0.5, -1e30)
        e = jnp.exp(s - jnp.max(s, axis=1, keepdims=True))
        part[2 + h // 4, :, h % 4 * 128:(h % 4 + 1) * 128] = (e / jnp.sum(e, axis=1, keepdims=True)).astype(BF16)
    for h in range(HEADS):
        vh = jnp.concatenate([vout[0, h], vout[1, h]], axis=0)
        ob[:, h * 128:(h + 1) * 128] = dot(part[2 + h // 4, :, h % 4 * 128:(h % 4 + 1) * 128], vh).astype(BF16)

    def d_copy(ph, c):
        return pltpu.make_async_remote_copy(
            part.at[c, theirs, :], d2d.at[c], d_s.at[lax.rem(c, 4)], d_r.at[c],
            device_id={"tp": partner}, device_id_type=MESH)

    def x_copy(ph, c):
        return pltpu.make_async_remote_copy(
            xsend.at[c], xrecv.at[ph, c], x_s.at[c], x_r.at[ph, c],
            device_id={"tp": cross}, device_id_type=MESH)

    def cols_of(c):
        return pl.ds(pl.multiple_of(c * CW, CW), CW)

    def a_copy(ph, c):
        blk = full.at[mine, cols_of(c)]
        return pltpu.make_async_remote_copy(
            blk, blk, a_s.at[lax.rem(c, 4)], a_r.at[c],
            device_id={"tp": partner}, device_id_type=MESH)

    def put(ph, c, val):
        part[c] = val.astype(BF16)
        d_copy(ph, c).start()

    def relay(ph, c):
        d_copy(ph, c).wait()
        xsend[c] = (part[c, mine, :].astype(F32) + d2d[c].astype(F32)).astype(BF16)
        x_copy(ph, c).start()

    def add_sq(rows, c):
        v = full[rows, cols_of(c)].astype(F32)
        v = v * v
        t = v[:, 0:128]
        for q in range(1, CW // 128):
            t = t + v[:, q * 128:(q + 1) * 128]
        ssq[rows, :] += t

    def finish_own(ph, c):
        x_copy(ph, c).wait()
        s = xsend[c].astype(F32) + xrecv[ph, c].astype(F32)
        full[mine, cols_of(c)] = s.astype(BF16)
        a_copy(ph, c).start()
        add_sq(mine, c)

    def finish_other(ph, c):
        a_copy(ph, c).wait()
        add_sq(theirs, c)

    ssq[...] = jnp.zeros_like(ssq)
    lag = 2
    for c in range(4):
        stream(12 + c).wait()
        for half in range(2):
            cc = 2 * c + half
            put(0, cc, dot(ob[...], slot(12 + c)[:, half * CW:(half + 1) * CW]))
            if cc >= lag:
                relay(0, cc - lag)

    _ph('xpose')
    @pl.loop(0, 2 * NTB)
    def _(j):
        with jax.named_scope('gwait'):
            gu_wait(j)
        s, m, n = lax.rem(j, NS), j // NTB, lax.rem(j, NTB)
        cols = pl.ds(pl.multiple_of(n * TB, TB), TB)
        _tr = jax.named_scope('tr')
        _tr.__enter__()
        for k in range(D // TB):
            blk = stg[s, :, k * TB:(k + 1) * TB]
            if k % 2 == 0:
                t = blk.T
            else:
                t = dot_t(eye[...], blk).astype(BF16)
            wgu[m, k * TB:(k + 1) * TB, cols] = t
        _tr.__exit__(None, None, None)

        @pl.when(j + NS < 2 * NTB)
        def _():
            gu_start(j + NS)

        @pl.when(j < lag)
        def _():
            relay(0, NC - lag + j)

        @pl.when((j >= 6) & (lax.rem(j, 2) == 0))
        def _():
            with jax.named_scope('fown'):
                finish_own(0, (j - 6) // 2)

        @pl.when((j >= 9) & (lax.rem(j, 2) == 1))
        def _():
            with jax.named_scope('foth'):
                finish_other(0, (j - 9) // 2)

    finish_other(0, NC - 1)

    _ph('norm1')
    rs1 = row_scale(ssq)

    for c in range(NC):
        add_norm(xh, full, rs1, ga32, c)


    def gate_up(start, width, keep):
        g = dot(xh[:, :D], wgu[0, :, pl.ds(start, width)])
        u = dot(xh[:, :D], wgu[1, :, pl.ds(start, width)])
        v = (g * jax.nn.sigmoid(g) * u).astype(BF16)
        act[:, pl.ds(start, keep)] = v[:, :keep]

    gate_up(0, NT, NT)
    down_copy(0).start()
    down_copy(1).start()

    @pl.loop(1, FF // NT)
    def _(n):
        gate_up(pl.multiple_of(n * NT, NT), NT, NT)

        @pl.when(n < NC // 2)
        def _():
            down_copy(2 * n).start()
            down_copy(2 * n + 1).start()

    tail = FF // NT * NT
    gate_up(tail, FFP - tail, FF - tail)
    ssq[...] = jnp.zeros_like(ssq)

    _ph('down')
    lag2 = 1

    @pl.loop(0, NC)
    def _(c):
        down_copy(c).wait()
        put(1, c, dot(act[...], wgu[lax.rem(c, 2), :FFP, down_cols(c)]))

        @pl.when(c >= lag2)
        def _():
            relay(1, c - lag2)

    _ph('relay_tail')
    for cc in range(NC - lag2, NC):
        relay(1, cc)

    _ph('finish2')
    @pl.loop(0, NC)
    def _(c):
        finish_own(1, c)

        @pl.when(c > 0)
        def _():
            finish_other(1, c - 1)

    finish_other(1, NC - 1)
    _ph('end')


def store_kernel(h, m, ssq, g32, kc, vc, y_h, kc_h, vc_h, y, sem):
    kv = [pltpu.make_async_copy(a, b, sem.at[i]) for i, (a, b) in enumerate(((kc, kc_h), (vc, vc_h)))]
    for copy in kv:
        copy.start()
    rs = row_scale(ssq)
    blocks = []
    for c in range(NC):
        for q in range(CW // 128):
            cols = slice(c * CW + q * 128, c * CW + (q + 1) * 128)
            r = c * (CW // 128) + q
            v = m[:, cols].astype(F32) * rs * g32[r:r + 1, :]
            y[:, cols] = (h[:, cols].astype(F32) + v).astype(BF16)
        cols = pl.ds(c * CW, CW)
        blocks.append(pltpu.make_async_copy(y.at[:, cols], y_h.at[:, cols], sem.at[2 + c]))
        blocks[-1].start()
    for copy in kv + blocks:
        copy.wait()


def solution(mesh):
    tables = rope_tables()

    def local_layer(tokens, seq_lens, w_q, w_k, w_v, w_o, g_q, g_k, g_attn, g_mlp, w_gate, w_up, w_down):
        vmem = pl.BlockSpec(memory_space=pltpu.VMEM)
        anyspace = pl.BlockSpec(memory_space=pl.ANY)
        dma = pltpu.SemaphoreType.DMA
        outs = pl.pallas_call(
            kernel,
            out_shape=(
                pltpu.VMEM((ROWS, DW), BF16),
                pltpu.VMEM((ROWS, D), BF16),
                pltpu.VMEM((ROWS, 128), F32),
                pltpu.VMEM((D // 128, 128), F32),
                pltpu.VMEM((PROMPTS, HEADS, SEQ, HEAD_DIM), BF16),
                pltpu.VMEM((PROMPTS, HEADS, SEQ, HEAD_DIM), BF16),
            ),
            in_specs=[anyspace] * 14,
            out_specs=(vmem,) * 6,
            scratch_shapes=[
                pltpu.VMEM((NS, TB, D), BF16),
                pltpu.VMEM((2, D, FFW), BF16),
                pltpu.VMEM((3, ROWS, QW), F32),
                pltpu.VMEM((ROWS, QW), BF16),
                pltpu.VMEM((NC, ROWS, CW), BF16),
                pltpu.VMEM((NC, HALF, CW), BF16),
                pltpu.VMEM((NC, HALF, CW), BF16),
                pltpu.VMEM((2, NC, HALF, CW), BF16),
                pltpu.VMEM((ROWS, FFP), BF16),
                pltpu.VMEM((2, ROWS, HEAD_DIM), F32),
                pltpu.VMEM((QW // 128, 128), BF16),
                pltpu.VMEM((QW // 128, 128), BF16),
                pltpu.VMEM((D // 128, 128), BF16),
                pltpu.VMEM((D // 128, 128), BF16),
                pltpu.VMEM((D // 128, 128), F32),
                pltpu.VMEM((8, 128), F32),
                pltpu.VMEM((3, 8, 128), F32),
                pltpu.VMEM((TB, TB), BF16),
                pltpu.SMEM((PROMPTS,), jnp.int32),
                dma((11,)), dma((3,)), dma((3,)),
                dma((4,)), dma((NC,)), dma((NC,)), dma((2, NC)), dma((4,)), dma((NC,)),
            ],
            compiler_params=pltpu.CompilerParams(
                collective_id=0, has_side_effects=True, vmem_limit_bytes=VMEM_LIMIT),
            name="layer",
        )(seq_lens, tokens.reshape(ROWS, D), w_q, w_k, w_v, w_o,
          g_q.reshape(-1, 128), g_k.reshape(-1, 128), g_attn.reshape(-1, 128), g_mlp.reshape(-1, 128),
          w_gate.T, w_up.T, w_down, jnp.asarray(tables))
        outs = [pltpu.with_memory_space_constraint(o, pltpu.VMEM) for o in outs]
        y, kc, vc = pl.pallas_call(
            store_kernel,
            out_shape=(
                jax.ShapeDtypeStruct((ROWS, D), BF16),
                jax.ShapeDtypeStruct((PROMPTS, HEADS, SEQ, HEAD_DIM), BF16),
                jax.ShapeDtypeStruct((PROMPTS, HEADS, SEQ, HEAD_DIM), BF16),
            ),
            in_specs=[vmem] * 6,
            out_specs=(anyspace,) * 3,
            scratch_shapes=[pltpu.VMEM((ROWS, D), BF16), dma((2 + NC,))],
            compiler_params=pltpu.CompilerParams(vmem_limit_bytes=3 * 2**19),
            name="store",
        )(*outs)
        return y.reshape(tokens.shape), kc, vc

    return jax.shard_map(local_layer, mesh=mesh, in_specs=(P('dp', None, None), P('dp'), P(None, 'tp'), P(None, 'tp'), P(None, 'tp'), P('tp', None), P('tp'), P('tp'), P(), P(), P(None, 'tp'), P(None, 'tp'), P('tp', None)), out_specs=(P('dp', None, None), P('dp', 'tp', None, None), P('dp', 'tp', None, None)), check_vma=False)
```

```python
import functools

import jax
import jax.numpy as jnp
import numpy as np
from jax import lax
from jax.experimental import pallas as pl
from jax.experimental.pallas import tpu as pltpu
from jax.sharding import PartitionSpec as P

HEAD_DIM = 128
ROPE_BASE = 500000.0
NORM_EPS = 1e-6

SEQ = 64
PROMPTS = 2
ROWS = SEQ * PROMPTS
HALF = ROWS // 2
D = 4096
QW = 1024
HEADS = QW // HEAD_DIM
FF = 2752
FFP = 2816
FFW = FFP + 128
DW = D + 128
KC = 1024
CW = 512
NC = D // CW
TB = 256
NTB = FFP // TB
NS = 4
DEPTH = 4
NEXT = {i: (i + 4,) for i in range(8)}
NEXT.update({9: (12,), 10: (13, 14), 11: (15,)})
NT = 512

VMEM_LIMIT = 61 * 2**20

F32 = jnp.float32
BF16 = jnp.bfloat16
MESH = pl.DeviceIdType.MESH


def rope_tables():
    half = HEAD_DIM // 2
    inv_freq = ROPE_BASE ** (-2.0 * np.arange(half, dtype=np.float64) / HEAD_DIM)
    inv_freq = inv_freq.astype(np.float32)
    angles = np.arange(SEQ, dtype=np.float32)[:, None] * inv_freq[None, :]
    cos = np.cos(angles.astype(np.float64)).astype(np.float32)
    sin = np.sin(angles.astype(np.float64)).astype(np.float32)
    cos2 = np.concatenate([cos, cos], axis=1)
    sin2 = np.concatenate([-sin, sin], axis=1)
    return np.stack([np.tile(cos2, (PROMPTS, 1)), np.tile(sin2, (PROMPTS, 1))])


def dot(a, b):
    return jnp.dot(a, b, preferred_element_type=F32)


def dot_t(a, b):
    return lax.dot_general(a, b, (((1,), (1,)), ((), ())), preferred_element_type=F32)


def row_scale(ssq):
    return lax.rsqrt(jnp.sum(ssq[...], axis=1, keepdims=True) * (1.0 / D) + NORM_EPS)


def add_norm(base, branch, rs, g32, c):
    for q in range(CW // 128):
        col = c * CW + q * 128
        cols = pl.ds(col if isinstance(c, int) else pl.multiple_of(col, 128), 128)
        v = branch[:, cols].astype(F32) * rs * g32[pl.ds(c * (CW // 128) + q, 1), :]
        base[:, cols] = (base[:, cols].astype(F32) + v).astype(BF16)


_cur = []


def _ph(name):
    if _cur:
        _cur.pop().__exit__(None, None, None)
    if name != 'end':
        sc = jax.named_scope(name)
        sc.__enter__()
        _cur.append(sc)


def kernel(lens_h, tok, wq, wk, wv, wo, gq_h, gk_h, ga_h, gm_h, wg, wu, wd, tab_h,
           xh, full, ssq, gm32, kout, vout,
           stg, wgu, acc, ob, part, d2d, xsend, xrecv, act,
           tab, gq, gk, ga, gm, ga32, st, st_recv, eye, lens,
           sem_w, st_s, st_r,
           d_s, d_r, x_s, x_r, a_s, a_r):
    me = lax.axis_index("tp")
    core = lax.rem(me, 2)
    partner = me + 1 - 2 * core
    cross = lax.rem(me + 2, 4)
    mine = pl.ds(pl.multiple_of(core * HALF, HALF), HALF)
    theirs = pl.ds(pl.multiple_of((1 - core) * HALF, HALF), HALF)
    local = pltpu.make_async_copy

    small = [(tok, xh.at[:, pl.ds(0, D)]), (tab_h, tab), (gq_h, gq), (gk_h, gk), (ga_h, ga), (gm_h, gm), (lens_h, lens)]

    def in_copy(i):
        return local(small[i][0], small[i][1], sem_w.at[4 + i])

    def slot(i):
        i = i % 8
        return wgu.at[1, pl.ds((i % 4) * KC, KC), pl.ds((i // 4) * KC, KC)]

    qkv = [wq, wk, wv]

    def stream(i):
        if i < 12:
            src = qkv[i // 4].at[pl.ds((i % 4) * KC, KC), :]
        else:
            src = wo.at[:, pl.ds((i - 12) * KC, KC)]
        return local(src, slot(i), sem_w.at[i % DEPTH])

    def gu_copy(w, n, s):
        rows = TB if n < NTB - 1 else FF - TB * (NTB - 1)
        return local(w.at[pl.ds(n * TB, rows), :], stg.at[s, pl.ds(0, rows), :], sem_w.at[4 + s])

    def gu_start(j):
        s = lax.rem(j, NS)
        n = lax.rem(j, NTB)
        for m, w in enumerate((wg, wu)):
            @pl.when((j // NTB == m) & (n < NTB - 1))
            def _():
                rows = pl.ds(pl.multiple_of(n * TB, TB), TB)
                local(w.at[rows, :], stg.at[s], sem_w.at[4 + s]).start()

            @pl.when((j // NTB == m) & (n == NTB - 1))
            def _():
                gu_copy(w, NTB - 1, s).start()

    def gu_wait(j):
        s = lax.rem(j, NS)
        n = lax.rem(j, NTB)

        @pl.when(n < NTB - 1)
        def _():
            gu_copy(wg, 0, s).wait()

        @pl.when(n == NTB - 1)
        def _():
            gu_copy(wg, NTB - 1, s).wait()

    def down_cols(c):
        return pl.ds(pl.multiple_of(c // 2 * CW, CW), CW)

    def down_copy(c):
        return local(wd.at[:, pl.ds(pl.multiple_of(c * CW, CW), CW)],
                     wgu.at[lax.rem(c, 2), pl.ds(0, FF), down_cols(c)], sem_w.at[c])

    _ph('init')
    in_copy(0).start()
    stream(0).start()
    for i in range(1, 7):
        in_copy(i).start()
    for i in range(1, DEPTH):
        stream(i).start()

    barrier = pltpu.get_barrier_semaphore()
    for j in range(1, 4):
        pl.semaphore_signal(barrier, inc=1, device_id={"tp": lax.rem(me + j, 4)}, device_id_type=MESH)
    acc[...] = jnp.zeros_like(acc)
    st[...] = jnp.zeros_like(st)
    er = lax.broadcasted_iota(jnp.int32, (TB, TB), 0)
    ec = lax.broadcasted_iota(jnp.int32, (TB, TB), 1)
    eye[...] = (er == ec).astype(F32).astype(BF16)
    act[:, FF // 128 * 128:] = jnp.zeros((ROWS, FFP - FF // 128 * 128), BF16)
    _ph('wait_x')
    in_copy(0).wait()

    def qkv_step(i):
        stream(i).wait()
        w, k = i // 4, i % 4
        acc[w] += dot(xh[:, k * KC:(k + 1) * KC], slot(i)[...])
        for n in NEXT.get(i, ()):
            stream(n).start()

    _ph('qk')
    for i in range(8):
        qkv_step(i)
    _ph('ssq_send')
    for w in range(2):
        t = jnp.zeros((ROWS, 128), F32)
        for h in range(HEADS):
            v = acc[w, :, h * 128:(h + 1) * 128]
            t = t + v * v
        st[w:w + 1, :] = jnp.sum(t.T, axis=0, keepdims=True)
    pl.semaphore_wait(barrier, 3)

    def st_copy(j):
        return pltpu.make_async_remote_copy(
            st, st_recv.at[j - 1], st_s.at[j - 1], st_r.at[j - 1],
            device_id={"tp": lax.rem(me + j, 4)}, device_id_type=MESH)

    for j in range(1, 4):
        st_copy(j).start()
    _ph('v')
    for i in range(8, 11):
        qkv_step(i)
    for i in range(1, 7):
        in_copy(i).wait()
    ga32[...] = ga[...].astype(F32)
    gm32[...] = gm[...].astype(F32)
    gq32, gk32 = gq[...].astype(F32), gk[...].astype(F32)
    _ph('st_wait')
    for j in range(1, 4):
        st_copy(j).wait()

    _ph('attn')
    tot = st[...] + st_recv[0] + st_recv[1] + st_recv[2]
    rs = lax.rsqrt(tot * (1.0 / D) + NORM_EPS)
    rq = jnp.broadcast_to(rs[0:1, :], (ROWS, 128)).T
    rk = jnp.broadcast_to(rs[1:2, :], (ROWS, 128)).T
    cos, sin = tab[0], tab[1]

    def rope(v):
        return v * cos + pltpu.roll(v, 64, axis=1) * sin

    ri = lax.broadcasted_iota(jnp.int32, (ROWS, ROWS), 0)
    ci = lax.broadcasted_iota(jnp.int32, (ROWS, ROWS), 1)
    same = (ri < SEQ) == (ci < SEQ)
    limit = jnp.where(ci < SEQ, lens[0], lens[1] + SEQ)
    allowed = same & (ci <= ri) & (ci < limit)
    for h in range(HEADS):
        cols = slice(h * 128, (h + 1) * 128)
        part[h // 4, :, h % 4 * 128:(h % 4 + 1) * 128] = rope(acc[0, :, cols] * rq * gq32[h:h + 1]).astype(BF16)
        kh = rope(acc[1, :, cols] * rk * gk32[h:h + 1]).astype(BF16)
        kout[0, h] = kh[:SEQ]
        kout[1, h] = kh[SEQ:]
    for h in range(HEADS):
        kh = jnp.concatenate([kout[0, h], kout[1, h]], axis=0)
        s = jnp.where(allowed, dot_t(part[h // 4, :, h % 4 * 128:(h % 4 + 1) * 128], kh) * HEAD_DIM ** -0.5, -1e30)
        e = jnp.exp(s - jnp.max(s, axis=1, keepdims=True))
        part[2 + h // 4, :, h % 4 * 128:(h % 4 + 1) * 128] = (e / jnp.sum(e, axis=1, keepdims=True)).astype(BF16)
    _ph('v_last')
    qkv_step(11)
    for j in range(NS):
        gu_copy(wg, j, j).start()
    _ph('pv')
    for h in range(HEADS):
        vh = acc[2, :, h * 128:(h + 1) * 128].astype(BF16)
        vout[0, h] = vh[:SEQ]
        vout[1, h] = vh[SEQ:]
        ob[:, h * 128:(h + 1) * 128] = dot(part[2 + h // 4, :, h % 4 * 128:(h % 4 + 1) * 128], vh).astype(BF16)

    def d_copy(ph, c):
        return pltpu.make_async_remote_copy(
            part.at[c, theirs, :], d2d.at[c], d_s.at[lax.rem(c, 4)], d_r.at[c],
            device_id={"tp": partner}, device_id_type=MESH)

    def x_copy(ph, c):
        return pltpu.make_async_remote_copy(
            xsend.at[c], xrecv.at[ph, c], x_s.at[c], x_r.at[ph, c],
            device_id={"tp": cross}, device_id_type=MESH)

    def cols_of(c):
        return pl.ds(pl.multiple_of(c * CW, CW), CW)

    def a_copy(ph, c):
        blk = full.at[mine, cols_of(c)]
        return pltpu.make_async_remote_copy(
            blk, blk, a_s.at[lax.rem(c, 4)], a_r.at[c],
            device_id={"tp": partner}, device_id_type=MESH)

    def put(ph, c, val):
        part[c] = val.astype(BF16)
        d_copy(ph, c).start()

    def relay(ph, c):
        d_copy(ph, c).wait()
        xsend[c] = (part[c, mine, :].astype(F32) + d2d[c].astype(F32)).astype(BF16)
        x_copy(ph, c).start()

    def add_sq(rows, c):
        v = full[rows, cols_of(c)].astype(F32)
        v = v * v
        t = v[:, 0:128]
        for q in range(1, CW // 128):
            t = t + v[:, q * 128:(q + 1) * 128]
        ssq[rows, :] += t

    def finish_own(ph, c):
        x_copy(ph, c).wait()
        s = xsend[c].astype(F32) + xrecv[ph, c].astype(F32)
        full[mine, cols_of(c)] = s.astype(BF16)
        a_copy(ph, c).start()
        add_sq(mine, c)

    def finish_other(ph, c):
        a_copy(ph, c).wait()
        add_sq(theirs, c)

    _ph('wo')
    ssq[...] = jnp.zeros_like(ssq)
    lag = 3
    for c in range(4):
        stream(12 + c).wait()
        for half in range(2):
            cc = 2 * c + half
            put(0, cc, dot(ob[...], slot(12 + c)[:, half * CW:(half + 1) * CW]))
            if cc >= lag:
                relay(0, cc - lag)

    _ph('xpose')
    @pl.loop(0, 2 * NTB)
    def _(j):
        gu_wait(j)
        s, m, n = lax.rem(j, NS), j // NTB, lax.rem(j, NTB)
        cols = pl.ds(pl.multiple_of(n * TB, TB), TB)
        for k in range(D // TB):
            blk = stg[s, :, k * TB:(k + 1) * TB]
            if k % 2 == 0:
                t = blk.T
            else:
                t = dot_t(eye[...], blk).astype(BF16)
            wgu[m, k * TB:(k + 1) * TB, cols] = t

        @pl.when(j + NS < 2 * NTB)
        def _():
            gu_start(j + NS)

        @pl.when(j < lag)
        def _():
            relay(0, NC - lag + j)

        @pl.when((j >= 6) & (lax.rem(j, 2) == 0))
        def _():
            finish_own(0, (j - 6) // 2)

        @pl.when((j >= 9) & (lax.rem(j, 2) == 1))
        def _():
            finish_other(0, (j - 9) // 2)

    finish_other(0, NC - 1)

    _ph('norm1')
    rs1 = row_scale(ssq)

    for c in range(NC):
        add_norm(xh, full, rs1, ga32, c)


    def gate_up(start, width, keep):
        g = dot(xh[:, :D], wgu[0, :, pl.ds(start, width)])
        u = dot(xh[:, :D], wgu[1, :, pl.ds(start, width)])
        v = (g * jax.nn.sigmoid(g) * u).astype(BF16)
        act[:, pl.ds(start, keep)] = v[:, :keep]

    gate_up(0, NT, NT)
    down_copy(0).start()
    down_copy(1).start()

    @pl.loop(1, FF // NT)
    def _(n):
        gate_up(pl.multiple_of(n * NT, NT), NT, NT)

        @pl.when(n < NC // 2)
        def _():
            down_copy(2 * n).start()
            down_copy(2 * n + 1).start()

    tail = FF // NT * NT
    gate_up(tail, FFP - tail, FF - tail)
    ssq[...] = jnp.zeros_like(ssq)

    _ph('down')
    lag2 = 1

    @pl.loop(0, NC)
    def _(c):
        down_copy(c).wait()
        put(1, c, dot(act[...], wgu[lax.rem(c, 2), :FFP, down_cols(c)]))

        @pl.when(c >= lag2)
        def _():
            relay(1, c - lag2)

    _ph('relay_tail')
    for cc in range(NC - lag2, NC):
        relay(1, cc)

    _ph('finish2')
    @pl.loop(0, NC)
    def _(c):
        finish_own(1, c)

        @pl.when(c > 0)
        def _():
            finish_other(1, c - 1)

    finish_other(1, NC - 1)
    _ph('end')


def store_kernel(h, m, ssq, g32, kc, vc, y_h, kc_h, vc_h, y, sem):
    kv = [pltpu.make_async_copy(a, b, sem.at[i]) for i, (a, b) in enumerate(((kc, kc_h), (vc, vc_h)))]
    for copy in kv:
        copy.start()
    rs = row_scale(ssq)
    blocks = []
    for c in range(NC):
        for q in range(CW // 128):
            cols = slice(c * CW + q * 128, c * CW + (q + 1) * 128)
            r = c * (CW // 128) + q
            v = m[:, cols].astype(F32) * rs * g32[r:r + 1, :]
            y[:, cols] = (h[:, cols].astype(F32) + v).astype(BF16)
        cols = pl.ds(c * CW, CW)
        blocks.append(pltpu.make_async_copy(y.at[:, cols], y_h.at[:, cols], sem.at[2 + c]))
        blocks[-1].start()
    for copy in kv + blocks:
        copy.wait()


def solution(mesh):
    tables = rope_tables()

    def local_layer(tokens, seq_lens, w_q, w_k, w_v, w_o, g_q, g_k, g_attn, g_mlp, w_gate, w_up, w_down):
        vmem = pl.BlockSpec(memory_space=pltpu.VMEM)
        anyspace = pl.BlockSpec(memory_space=pl.ANY)
        dma = pltpu.SemaphoreType.DMA
        outs = pl.pallas_call(
            kernel,
            out_shape=(
                pltpu.VMEM((ROWS, DW), BF16),
                pltpu.VMEM((ROWS, D), BF16),
                pltpu.VMEM((ROWS, 128), F32),
                pltpu.VMEM((D // 128, 128), F32),
                pltpu.VMEM((PROMPTS, HEADS, SEQ, HEAD_DIM), BF16),
                pltpu.VMEM((PROMPTS, HEADS, SEQ, HEAD_DIM), BF16),
            ),
            in_specs=[anyspace] * 14,
            out_specs=(vmem,) * 6,
            scratch_shapes=[
                pltpu.VMEM((NS, TB, D), BF16),
                pltpu.VMEM((2, D, FFW), BF16),
                pltpu.VMEM((3, ROWS, QW), F32),
                pltpu.VMEM((ROWS, QW), BF16),
                pltpu.VMEM((NC, ROWS, CW), BF16),
                pltpu.VMEM((NC, HALF, CW), BF16),
                pltpu.VMEM((NC, HALF, CW), BF16),
                pltpu.VMEM((2, NC, HALF, CW), BF16),
                pltpu.VMEM((ROWS, FFP), BF16),
                pltpu.VMEM((2, ROWS, HEAD_DIM), F32),
                pltpu.VMEM((QW // 128, 128), BF16),
                pltpu.VMEM((QW // 128, 128), BF16),
                pltpu.VMEM((D // 128, 128), BF16),
                pltpu.VMEM((D // 128, 128), BF16),
                pltpu.VMEM((D // 128, 128), F32),
                pltpu.VMEM((8, 128), F32),
                pltpu.VMEM((3, 8, 128), F32),
                pltpu.VMEM((TB, TB), BF16),
                pltpu.SMEM((PROMPTS,), jnp.int32),
                dma((11,)), dma((3,)), dma((3,)),
                dma((4,)), dma((NC,)), dma((NC,)), dma((2, NC)), dma((4,)), dma((NC,)),
            ],
            compiler_params=pltpu.CompilerParams(
                collective_id=0, has_side_effects=True, vmem_limit_bytes=VMEM_LIMIT),
            name="layer",
        )(seq_lens, tokens.reshape(ROWS, D), w_q, w_k, w_v, w_o,
          g_q.reshape(-1, 128), g_k.reshape(-1, 128), g_attn.reshape(-1, 128), g_mlp.reshape(-1, 128),
          w_gate.T, w_up.T, w_down, jnp.asarray(tables))
        outs = [pltpu.with_memory_space_constraint(o, pltpu.VMEM) for o in outs]
        y, kc, vc = pl.pallas_call(
            store_kernel,
            out_shape=(
                jax.ShapeDtypeStruct((ROWS, D), BF16),
                jax.ShapeDtypeStruct((PROMPTS, HEADS, SEQ, HEAD_DIM), BF16),
                jax.ShapeDtypeStruct((PROMPTS, HEADS, SEQ, HEAD_DIM), BF16),
            ),
            in_specs=[vmem] * 6,
            out_specs=(anyspace,) * 3,
            scratch_shapes=[pltpu.VMEM((ROWS, D), BF16), dma((2 + NC,))],
            compiler_params=pltpu.CompilerParams(vmem_limit_bytes=3 * 2**19),
            name="store",
        )(*outs)
        return y.reshape(tokens.shape), kc, vc

    return jax.shard_map(local_layer, mesh=mesh, in_specs=(P('dp', None, None), P('dp'), P(None, 'tp'), P(None, 'tp'), P(None, 'tp'), P('tp', None), P('tp'), P('tp'), P(), P(), P(None, 'tp'), P(None, 'tp'), P('tp', None)), out_specs=(P('dp', None, None), P('dp', 'tp', None, None), P('dp', 'tp', None, None)), check_vma=False)
```

```python
import functools

import jax
import jax.numpy as jnp
import numpy as np
from jax import lax
from jax.experimental import pallas as pl
from jax.experimental.pallas import tpu as pltpu
from jax.sharding import PartitionSpec as P

HEAD_DIM = 128
ROPE_BASE = 500000.0
NORM_EPS = 1e-6

SEQ = 64
PROMPTS = 2
ROWS = SEQ * PROMPTS
HALF = ROWS // 2
D = 4096
QW = 1024
HEADS = QW // HEAD_DIM
FF = 2752
FFP = 2816
FFW = FFP + 128
DW = D + 128
KC = 1024
CW = 512
NC = D // CW
TB = 256
NTB = FFP // TB
NS = 4
DEPTH = 4
NEXT = {i: (i + 4,) for i in range(8)}
NEXT.update({9: (12,), 10: (13,), 11: (14, 15)})
NT = 512

VMEM_LIMIT = 61 * 2**20

F32 = jnp.float32
BF16 = jnp.bfloat16
MESH = pl.DeviceIdType.MESH


def rope_tables():
    half = HEAD_DIM // 2
    inv_freq = ROPE_BASE ** (-2.0 * np.arange(half, dtype=np.float64) / HEAD_DIM)
    inv_freq = inv_freq.astype(np.float32)
    angles = np.arange(SEQ, dtype=np.float32)[:, None] * inv_freq[None, :]
    cos = np.cos(angles.astype(np.float64)).astype(np.float32)
    sin = np.sin(angles.astype(np.float64)).astype(np.float32)
    cos2 = np.concatenate([cos, cos], axis=1)
    sin2 = np.concatenate([-sin, sin], axis=1)
    return np.stack([np.tile(cos2, (PROMPTS, 1)), np.tile(sin2, (PROMPTS, 1))])


def dot(a, b):
    return jnp.dot(a, b, preferred_element_type=F32)


def dot_t(a, b):
    return lax.dot_general(a, b, (((1,), (1,)), ((), ())), preferred_element_type=F32)


def row_scale(ssq):
    return lax.rsqrt(jnp.sum(ssq[...], axis=1, keepdims=True) * (1.0 / D) + NORM_EPS)


def add_norm(base, branch, rs, g32, c):
    for q in range(CW // 128):
        col = c * CW + q * 128
        cols = pl.ds(col if isinstance(c, int) else pl.multiple_of(col, 128), 128)
        v = branch[:, cols].astype(F32) * rs * g32[pl.ds(c * (CW // 128) + q, 1), :]
        base[:, cols] = (base[:, cols].astype(F32) + v).astype(BF16)


_cur = []


def _ph(name):
    if _cur:
        _cur.pop().__exit__(None, None, None)
    if name != 'end':
        sc = jax.named_scope(name)
        sc.__enter__()
        _cur.append(sc)


def kernel(lens_h, tok, wq, wk, wv, wo, gq_h, gk_h, ga_h, gm_h, wg, wu, wd, tab_h,
           xh, full, ssq, gm32, kout, vout,
           stg, wgu, acc, ob, part, d2d, xsend, xrecv, act,
           tab, gq, gk, ga, gm, ga32, st, st_recv, eye, lens, rolled,
           sem_w, st_s, st_r,
           d_s, d_r, x_s, x_r, a_s, a_r):
    me = lax.axis_index("tp")
    core = lax.rem(me, 2)
    partner = me + 1 - 2 * core
    cross = lax.rem(me + 2, 4)
    mine = pl.ds(pl.multiple_of(core * HALF, HALF), HALF)
    theirs = pl.ds(pl.multiple_of((1 - core) * HALF, HALF), HALF)
    local = pltpu.make_async_copy

    small = [(tok, xh.at[:, pl.ds(0, D)]), (tab_h, tab), (gq_h, gq), (gk_h, gk), (ga_h, ga), (gm_h, gm), (lens_h, lens)]

    def in_copy(i):
        return local(small[i][0], small[i][1], sem_w.at[4 + i])

    def slot(i):
        i = i % 8
        return wgu.at[1, pl.ds((i % 4) * KC, KC), pl.ds((i // 4) * KC, KC)]

    qkv = [wq, wk, wv]

    def stream(i):
        if i < 12:
            src = qkv[i // 4].at[pl.ds((i % 4) * KC, KC), :]
        else:
            src = wo.at[:, pl.ds((i - 12) * KC, KC)]
        return local(src, slot(i), sem_w.at[i % DEPTH])

    def gu_copy(w, n, s):
        rows = TB if n < NTB - 1 else FF - TB * (NTB - 1)
        return local(w.at[pl.ds(n * TB, rows), :], stg.at[s, pl.ds(0, rows), :], sem_w.at[4 + s])

    def gu_start(j):
        s = lax.rem(j, NS)
        n = lax.rem(j, NTB)
        for m, w in enumerate((wg, wu)):
            @pl.when((j // NTB == m) & (n < NTB - 1))
            def _():
                rows = pl.ds(pl.multiple_of(n * TB, TB), TB)
                local(w.at[rows, :], stg.at[s], sem_w.at[4 + s]).start()

            @pl.when((j // NTB == m) & (n == NTB - 1))
            def _():
                gu_copy(w, NTB - 1, s).start()

    def gu_wait(j):
        s = lax.rem(j, NS)
        n = lax.rem(j, NTB)

        @pl.when(n < NTB - 1)
        def _():
            gu_copy(wg, 0, s).wait()

        @pl.when(n == NTB - 1)
        def _():
            gu_copy(wg, NTB - 1, s).wait()

    def down_cols(c):
        return pl.ds(pl.multiple_of(c // 2 * CW, CW), CW)

    def down_copy(c):
        return local(wd.at[:, pl.ds(pl.multiple_of(c * CW, CW), CW)],
                     wgu.at[lax.rem(c, 2), pl.ds(0, FF), down_cols(c)], sem_w.at[c])

    _ph('init')
    in_copy(0).start()
    stream(0).start()
    for i in range(1, 7):
        in_copy(i).start()
    for i in range(1, DEPTH):
        stream(i).start()

    barrier = pltpu.get_barrier_semaphore()
    for j in range(1, 4):
        pl.semaphore_signal(barrier, inc=1, device_id={"tp": lax.rem(me + j, 4)}, device_id_type=MESH)
    acc[...] = jnp.zeros_like(acc)
    st[...] = jnp.zeros_like(st)
    er = lax.broadcasted_iota(jnp.int32, (TB, TB), 0)
    ec = lax.broadcasted_iota(jnp.int32, (TB, TB), 1)
    eye[...] = (er == ec).astype(F32).astype(BF16)
    act[:, FF // 128 * 128:] = jnp.zeros((ROWS, FFP - FF // 128 * 128), BF16)
    _ph('wait_x')
    in_copy(0).wait()

    def qkv_step(i):
        stream(i).wait()
        w, k = i // 4, i % 4
        acc[w] += dot(xh[:, k * KC:(k + 1) * KC], slot(i)[...])
        for n in NEXT.get(i, ()):
            stream(n).start()

    _ph('qk')
    for i in range(8):
        qkv_step(i)
    _ph('ssq_send')
    for w in range(2):
        t = jnp.zeros((ROWS, 128), F32)
        for h in range(HEADS):
            v = acc[w, :, h * 128:(h + 1) * 128]
            t = t + v * v
        st[w:w + 1, :] = jnp.sum(t.T, axis=0, keepdims=True)
    pl.semaphore_wait(barrier, 3)

    def st_copy(j):
        return pltpu.make_async_remote_copy(
            st, st_recv.at[j - 1], st_s.at[j - 1], st_r.at[j - 1],
            device_id={"tp": lax.rem(me + j, 4)}, device_id_type=MESH)

    for j in range(1, 4):
        st_copy(j).start()
    for w in range(2):
        for h in range(HEADS):
            cols = slice(h * 128, (h + 1) * 128)
            rolled[w, :, cols] = pltpu.roll(acc[w, :, cols], 64, axis=1)
    _ph('v')
    for i in range(8, 12):
        qkv_step(i)
    for i in range(1, 7):
        in_copy(i).wait()
    for j in range(NS):
        gu_copy(wg, j, j).start()
    _ph('vout')
    ga32[...] = ga[...].astype(F32)
    gm32[...] = gm[...].astype(F32)
    gq32, gk32 = gq[...].astype(F32), gk[...].astype(F32)
    for h in range(HEADS):
        vh = acc[2, :, h * 128:(h + 1) * 128].astype(BF16)
        vout[0, h] = vh[:SEQ]
        vout[1, h] = vh[SEQ:]
    _ph('st_wait')
    for j in range(1, 4):
        st_copy(j).wait()

    _ph('attn')
    tot = st[...] + st_recv[0] + st_recv[1] + st_recv[2]
    rs = lax.rsqrt(tot * (1.0 / D) + NORM_EPS)
    rq = jnp.broadcast_to(rs[0:1, :], (ROWS, 128)).T
    rk = jnp.broadcast_to(rs[1:2, :], (ROWS, 128)).T
    cos, sin = tab[0], tab[1]

    gq32r, gk32r = pltpu.roll(gq32, 64, axis=1), pltpu.roll(gk32, 64, axis=1)

    def rope(w, h, r, g, gr):
        cols = slice(h * 128, (h + 1) * 128)
        return (acc[w, :, cols] * r * g[h:h + 1] * cos + rolled[w, :, cols] * r * gr[h:h + 1] * sin).astype(BF16)

    ri = lax.broadcasted_iota(jnp.int32, (ROWS, ROWS), 0)
    ci = lax.broadcasted_iota(jnp.int32, (ROWS, ROWS), 1)
    same = (ri < SEQ) == (ci < SEQ)
    limit = jnp.where(ci < SEQ, lens[0], lens[1] + SEQ)
    allowed = same & (ci <= ri) & (ci < limit)
    for h in range(HEADS):
        part[h // 4, :, h % 4 * 128:(h % 4 + 1) * 128] = rope(0, h, rq, gq32, gq32r)
        kh = rope(1, h, rk, gk32, gk32r)
        kout[0, h] = kh[:SEQ]
        kout[1, h] = kh[SEQ:]
    for h in range(HEADS):
        kh = jnp.concatenate([kout[0, h], kout[1, h]], axis=0)
        s = jnp.where(allowed, dot_t(part[h // 4, :, h % 4 * 128:(h % 4 + 1) * 128], kh) * HEAD_DIM ** -0.5, -1e30)
        e = jnp.exp(s - jnp.max(s, axis=1, keepdims=True))
        part[2 + h // 4, :, h % 4 * 128:(h % 4 + 1) * 128] = (e / jnp.sum(e, axis=1, keepdims=True)).astype(BF16)
    for h in range(HEADS):
        vh = jnp.concatenate([vout[0, h], vout[1, h]], axis=0)
        ob[:, h * 128:(h + 1) * 128] = dot(part[2 + h // 4, :, h % 4 * 128:(h % 4 + 1) * 128], vh).astype(BF16)

    def d_copy(ph, c):
        return pltpu.make_async_remote_copy(
            part.at[c, theirs, :], d2d.at[c], d_s.at[lax.rem(c, 4)], d_r.at[c],
            device_id={"tp": partner}, device_id_type=MESH)

    def x_copy(ph, c):
        return pltpu.make_async_remote_copy(
            xsend.at[c], xrecv.at[ph, c], x_s.at[c], x_r.at[ph, c],
            device_id={"tp": cross}, device_id_type=MESH)

    def cols_of(c):
        return pl.ds(pl.multiple_of(c * CW, CW), CW)

    def a_copy(ph, c):
        blk = full.at[mine, cols_of(c)]
        return pltpu.make_async_remote_copy(
            blk, blk, a_s.at[lax.rem(c, 4)], a_r.at[c],
            device_id={"tp": partner}, device_id_type=MESH)

    def put(ph, c, val):
        part[c] = val.astype(BF16)
        d_copy(ph, c).start()

    def relay(ph, c):
        d_copy(ph, c).wait()
        xsend[c] = (part[c, mine, :].astype(F32) + d2d[c].astype(F32)).astype(BF16)
        x_copy(ph, c).start()

    def add_sq(rows, c):
        v = full[rows, cols_of(c)].astype(F32)
        v = v * v
        t = v[:, 0:128]
        for q in range(1, CW // 128):
            t = t + v[:, q * 128:(q + 1) * 128]
        ssq[rows, :] += t

    def finish_own(ph, c):
        x_copy(ph, c).wait()
        s = xsend[c].astype(F32) + xrecv[ph, c].astype(F32)
        full[mine, cols_of(c)] = s.astype(BF16)
        a_copy(ph, c).start()
        add_sq(mine, c)

    def finish_other(ph, c):
        a_copy(ph, c).wait()
        add_sq(theirs, c)

    _ph('wo')
    ssq[...] = jnp.zeros_like(ssq)
    lag = 3
    for c in range(4):
        stream(12 + c).wait()
        for half in range(2):
            cc = 2 * c + half
            put(0, cc, dot(ob[...], slot(12 + c)[:, half * CW:(half + 1) * CW]))
            if cc >= lag:
                relay(0, cc - lag)

    _ph('xpose')
    @pl.loop(0, 2 * NTB)
    def _(j):
        gu_wait(j)
        s, m, n = lax.rem(j, NS), j // NTB, lax.rem(j, NTB)
        cols = pl.ds(pl.multiple_of(n * TB, TB), TB)
        for k in range(D // TB):
            blk = stg[s, :, k * TB:(k + 1) * TB]
            if k % 2 == 0:
                t = blk.T
            else:
                t = dot_t(eye[...], blk).astype(BF16)
            wgu[m, k * TB:(k + 1) * TB, cols] = t

        @pl.when(j + NS < 2 * NTB)
        def _():
            gu_start(j + NS)

        @pl.when(j < lag)
        def _():
            relay(0, NC - lag + j)

        @pl.when((j >= 6) & (lax.rem(j, 2) == 0))
        def _():
            finish_own(0, (j - 6) // 2)

        @pl.when((j >= 9) & (lax.rem(j, 2) == 1))
        def _():
            finish_other(0, (j - 9) // 2)

    finish_other(0, NC - 1)

    _ph('norm1')
    rs1 = row_scale(ssq)

    for c in range(NC):
        add_norm(xh, full, rs1, ga32, c)


    def gate_up(start, width, keep):
        g = dot(xh[:, :D], wgu[0, :, pl.ds(start, width)])
        u = dot(xh[:, :D], wgu[1, :, pl.ds(start, width)])
        v = (g * jax.nn.sigmoid(g) * u).astype(BF16)
        act[:, pl.ds(start, keep)] = v[:, :keep]

    for n in range(FF // NT):
        gate_up(n * NT, NT, NT)
        if n < NC // 2:
            down_copy(2 * n).start()
            down_copy(2 * n + 1).start()

    tail = FF // NT * NT
    gate_up(tail, FFP - tail, FF - tail)
    ssq[...] = jnp.zeros_like(ssq)

    _ph('down')
    lag2 = 1

    @pl.loop(0, NC)
    def _(c):
        down_copy(c).wait()
        put(1, c, dot(act[...], wgu[lax.rem(c, 2), :FFP, down_cols(c)]))

        @pl.when(c >= lag2)
        def _():
            relay(1, c - lag2)

    _ph('relay_tail')
    for cc in range(NC - lag2, NC):
        relay(1, cc)

    _ph('finish2')
    @pl.loop(0, NC)
    def _(c):
        finish_own(1, c)

        @pl.when(c > 0)
        def _():
            finish_other(1, c - 1)

    finish_other(1, NC - 1)
    _ph('end')


def store_kernel(h, m, ssq, g32, kc, vc, y_h, kc_h, vc_h, y, sem):
    kv = [pltpu.make_async_copy(a, b, sem.at[i]) for i, (a, b) in enumerate(((kc, kc_h), (vc, vc_h)))]
    for copy in kv:
        copy.start()
    rs = row_scale(ssq)
    blocks = []
    for c in range(NC):
        for q in range(CW // 128):
            cols = slice(c * CW + q * 128, c * CW + (q + 1) * 128)
            r = c * (CW // 128) + q
            v = m[:, cols].astype(F32) * rs * g32[r:r + 1, :]
            y[:, cols] = (h[:, cols].astype(F32) + v).astype(BF16)
        cols = pl.ds(c * CW, CW)
        blocks.append(pltpu.make_async_copy(y.at[:, cols], y_h.at[:, cols], sem.at[2 + c]))
        blocks[-1].start()
    for copy in kv + blocks:
        copy.wait()


def solution(mesh):
    tables = rope_tables()

    def local_layer(tokens, seq_lens, w_q, w_k, w_v, w_o, g_q, g_k, g_attn, g_mlp, w_gate, w_up, w_down):
        vmem = pl.BlockSpec(memory_space=pltpu.VMEM)
        anyspace = pl.BlockSpec(memory_space=pl.ANY)
        dma = pltpu.SemaphoreType.DMA
        outs = pl.pallas_call(
            kernel,
            out_shape=(
                pltpu.VMEM((ROWS, DW), BF16),
                pltpu.VMEM((ROWS, D), BF16),
                pltpu.VMEM((ROWS, 128), F32),
                pltpu.VMEM((D // 128, 128), F32),
                pltpu.VMEM((PROMPTS, HEADS, SEQ, HEAD_DIM), BF16),
                pltpu.VMEM((PROMPTS, HEADS, SEQ, HEAD_DIM), BF16),
            ),
            in_specs=[anyspace] * 14,
            out_specs=(vmem,) * 6,
            scratch_shapes=[
                pltpu.VMEM((NS, TB, D), BF16),
                pltpu.VMEM((2, D, FFW), BF16),
                pltpu.VMEM((3, ROWS, QW), F32),
                pltpu.VMEM((ROWS, QW), BF16),
                pltpu.VMEM((NC, ROWS, CW), BF16),
                pltpu.VMEM((NC, HALF, CW), BF16),
                pltpu.VMEM((NC, HALF, CW), BF16),
                pltpu.VMEM((2, NC, HALF, CW), BF16),
                pltpu.VMEM((ROWS, FFP), BF16),
                pltpu.VMEM((2, ROWS, HEAD_DIM), F32),
                pltpu.VMEM((QW // 128, 128), BF16),
                pltpu.VMEM((QW // 128, 128), BF16),
                pltpu.VMEM((D // 128, 128), BF16),
                pltpu.VMEM((D // 128, 128), BF16),
                pltpu.VMEM((D // 128, 128), F32),
                pltpu.VMEM((8, 128), F32),
                pltpu.VMEM((3, 8, 128), F32),
                pltpu.VMEM((TB, TB), BF16),
                pltpu.SMEM((PROMPTS,), jnp.int32),
                pltpu.VMEM((2, ROWS, QW), F32),
                dma((11,)), dma((3,)), dma((3,)),
                dma((4,)), dma((NC,)), dma((NC,)), dma((2, NC)), dma((4,)), dma((NC,)),
            ],
            compiler_params=pltpu.CompilerParams(
                collective_id=0, has_side_effects=True, vmem_limit_bytes=VMEM_LIMIT),
            name="layer",
        )(seq_lens, tokens.reshape(ROWS, D), w_q, w_k, w_v, w_o,
          g_q.reshape(-1, 128), g_k.reshape(-1, 128), g_attn.reshape(-1, 128), g_mlp.reshape(-1, 128),
          w_gate.T, w_up.T, w_down, jnp.asarray(tables))
        outs = [pltpu.with_memory_space_constraint(o, pltpu.VMEM) for o in outs]
        y, kc, vc = pl.pallas_call(
            store_kernel,
            out_shape=(
                jax.ShapeDtypeStruct((ROWS, D), BF16),
                jax.ShapeDtypeStruct((PROMPTS, HEADS, SEQ, HEAD_DIM), BF16),
                jax.ShapeDtypeStruct((PROMPTS, HEADS, SEQ, HEAD_DIM), BF16),
            ),
            in_specs=[vmem] * 6,
            out_specs=(anyspace,) * 3,
            scratch_shapes=[pltpu.VMEM((ROWS, D), BF16), dma((2 + NC,))],
            compiler_params=pltpu.CompilerParams(vmem_limit_bytes=3 * 2**19),
            name="store",
        )(*outs)
        return y.reshape(tokens.shape), kc, vc

    return jax.shard_map(local_layer, mesh=mesh, in_specs=(P('dp', None, None), P('dp'), P(None, 'tp'), P(None, 'tp'), P(None, 'tp'), P('tp', None), P('tp'), P('tp'), P(), P(), P(None, 'tp'), P(None, 'tp'), P('tp', None)), out_specs=(P('dp', None, None), P('dp', 'tp', None, None), P('dp', 'tp', None, None)), check_vma=False)
```

```python
import functools

import jax
import jax.numpy as jnp
import numpy as np
from jax import lax
from jax.experimental import pallas as pl
from jax.experimental.pallas import tpu as pltpu
from jax.sharding import PartitionSpec as P

HEAD_DIM = 128
ROPE_BASE = 500000.0
NORM_EPS = 1e-6

SEQ = 64
PROMPTS = 2
ROWS = SEQ * PROMPTS
HALF = ROWS // 2
D = 4096
QW = 1024
HEADS = QW // HEAD_DIM
FF = 2752
FFP = 2816
FFW = FFP + 128
DW = D + 128
KC = 1024
CW = 512
NC = D // CW
TB = 256
NTB = FFP // TB
NS = 4
DEPTH = 4
NEXT = {i: (i + 4,) for i in range(8)}
NEXT.update({9: (12,), 10: (13,), 11: (14, 15)})
NT = 512

VMEM_LIMIT = 61 * 2**20

F32 = jnp.float32
BF16 = jnp.bfloat16
MESH = pl.DeviceIdType.MESH


def rope_tables():
    half = HEAD_DIM // 2
    inv_freq = ROPE_BASE ** (-2.0 * np.arange(half, dtype=np.float64) / HEAD_DIM)
    inv_freq = inv_freq.astype(np.float32)
    angles = np.arange(SEQ, dtype=np.float32)[:, None] * inv_freq[None, :]
    cos = np.cos(angles.astype(np.float64)).astype(np.float32)
    sin = np.sin(angles.astype(np.float64)).astype(np.float32)
    cos2 = np.concatenate([cos, cos], axis=1)
    sin2 = np.concatenate([-sin, sin], axis=1)
    return np.stack([np.tile(cos2, (PROMPTS, 1)), np.tile(sin2, (PROMPTS, 1))])


def dot(a, b):
    return jnp.dot(a, b, preferred_element_type=F32)


def dot_t(a, b):
    return lax.dot_general(a, b, (((1,), (1,)), ((), ())), preferred_element_type=F32)


def row_scale(ssq):
    return lax.rsqrt(jnp.sum(ssq[...], axis=1, keepdims=True) * (1.0 / D) + NORM_EPS)


def add_norm(base, branch, rs, g32, c):
    for q in range(CW // 128):
        col = c * CW + q * 128
        cols = pl.ds(col if isinstance(c, int) else pl.multiple_of(col, 128), 128)
        v = branch[:, cols].astype(F32) * rs * g32[pl.ds(c * (CW // 128) + q, 1), :]
        base[:, cols] = (base[:, cols].astype(F32) + v).astype(BF16)


_cur = []


def _ph(name):
    if _cur:
        _cur.pop().__exit__(None, None, None)
    if name != 'end':
        sc = jax.named_scope(name)
        sc.__enter__()
        _cur.append(sc)


def kernel(lens_h, tok, wq, wk, wv, wo, gq_h, gk_h, ga_h, gm_h, wg, wu, wd, tab_h,
           xh, full, ssq, gm32, kout, vout,
           stg, wgu, acc, ob, part, d2d, xsend, xrecv, act,
           tab, gq, gk, ga, gm, ga32, st, st_recv, eye, lens, rolled,
           sem_w, st_s, st_r,
           d_s, d_r, x_s, x_r, a_s, a_r):
    me = lax.axis_index("tp")
    core = lax.rem(me, 2)
    partner = me + 1 - 2 * core
    cross = lax.rem(me + 2, 4)
    mine = pl.ds(pl.multiple_of(core * HALF, HALF), HALF)
    theirs = pl.ds(pl.multiple_of((1 - core) * HALF, HALF), HALF)
    local = pltpu.make_async_copy

    small = [(tok, xh.at[:, pl.ds(0, D)]), (tab_h, tab), (gq_h, gq), (gk_h, gk), (ga_h, ga), (gm_h, gm), (lens_h, lens)]

    def in_copy(i):
        return local(small[i][0], small[i][1], sem_w.at[4 + i])

    def slot(i):
        i = i % 8
        return wgu.at[1, pl.ds((i % 4) * KC, KC), pl.ds((i // 4) * KC, KC)]

    qkv = [wq, wk, wv]

    def stream(i):
        if i < 12:
            src = qkv[i // 4].at[pl.ds((i % 4) * KC, KC), :]
        else:
            src = wo.at[:, pl.ds((i - 12) * KC, KC)]
        return local(src, slot(i), sem_w.at[i % DEPTH])

    def gu_copy(w, n, s):
        rows = TB if n < NTB - 1 else FF - TB * (NTB - 1)
        return local(w.at[pl.ds(n * TB, rows), :], stg.at[s, pl.ds(0, rows), :], sem_w.at[4 + s])

    def gu_start(j):
        s = lax.rem(j, NS)
        n = lax.rem(j, NTB)
        for m, w in enumerate((wg, wu)):
            @pl.when((j // NTB == m) & (n < NTB - 1))
            def _():
                rows = pl.ds(pl.multiple_of(n * TB, TB), TB)
                local(w.at[rows, :], stg.at[s], sem_w.at[4 + s]).start()

            @pl.when((j // NTB == m) & (n == NTB - 1))
            def _():
                gu_copy(w, NTB - 1, s).start()

    def gu_wait(j):
        s = lax.rem(j, NS)
        n = lax.rem(j, NTB)

        @pl.when(n < NTB - 1)
        def _():
            gu_copy(wg, 0, s).wait()

        @pl.when(n == NTB - 1)
        def _():
            gu_copy(wg, NTB - 1, s).wait()

    def down_copy(c):
        return local(wd.at[:, pl.ds(c * CW, CW)],
                     wgu.at[c % 2, pl.ds(0, FF), pl.ds(c // 2 * CW, CW)], sem_w.at[c])

    _ph('init')
    in_copy(0).start()
    stream(0).start()
    for i in range(1, 7):
        in_copy(i).start()
    for i in range(1, DEPTH):
        stream(i).start()

    barrier = pltpu.get_barrier_semaphore()
    for j in range(1, 4):
        pl.semaphore_signal(barrier, inc=1, device_id={"tp": lax.rem(me + j, 4)}, device_id_type=MESH)
    acc[...] = jnp.zeros_like(acc)
    st[...] = jnp.zeros_like(st)
    er = lax.broadcasted_iota(jnp.int32, (TB, TB), 0)
    ec = lax.broadcasted_iota(jnp.int32, (TB, TB), 1)
    eye[...] = (er == ec).astype(F32).astype(BF16)
    act[:, FF // 128 * 128:] = jnp.zeros((ROWS, FFP - FF // 128 * 128), BF16)
    _ph('wait_x')
    in_copy(0).wait()

    def qkv_step(i):
        stream(i).wait()
        w, k = i // 4, i % 4
        acc[w] += dot(xh[:, k * KC:(k + 1) * KC], slot(i)[...])
        for n in NEXT.get(i, ()):
            stream(n).start()

    _ph('qk')
    for i in range(8):
        qkv_step(i)
    _ph('ssq_send')
    for w in range(2):
        t = jnp.zeros((ROWS, 128), F32)
        for h in range(HEADS):
            v = acc[w, :, h * 128:(h + 1) * 128]
            t = t + v * v
        st[w:w + 1, :] = jnp.sum(t.T, axis=0, keepdims=True)
    pl.semaphore_wait(barrier, 3)

    def st_copy(j):
        return pltpu.make_async_remote_copy(
            st, st_recv.at[j - 1], st_s.at[j - 1], st_r.at[j - 1],
            device_id={"tp": lax.rem(me + j, 4)}, device_id_type=MESH)

    for j in range(1, 4):
        st_copy(j).start()
    _ph('v')
    qkv_step(8)
    for w in range(2):
        for h in range(HEADS):
            cols = slice(h * 128, (h + 1) * 128)
            rolled[w, :, cols] = pltpu.roll(acc[w, :, cols], 64, axis=1)
    for i in range(9, 12):
        qkv_step(i)
    for i in range(1, 7):
        in_copy(i).wait()
    for j in range(NS):
        gu_copy(wg, j, j).start()
    _ph('vout')
    ga32[...] = ga[...].astype(F32)
    gm32[...] = gm[...].astype(F32)
    gq32, gk32 = gq[...].astype(F32), gk[...].astype(F32)
    for h in range(HEADS):
        vh = acc[2, :, h * 128:(h + 1) * 128].astype(BF16)
        vout[0, h] = vh[:SEQ]
        vout[1, h] = vh[SEQ:]
    _ph('st_wait')
    for j in range(1, 4):
        st_copy(j).wait()

    _ph('attn')
    tot = st[...] + st_recv[0] + st_recv[1] + st_recv[2]
    rs = lax.rsqrt(tot * (1.0 / D) + NORM_EPS)
    rq = jnp.broadcast_to(rs[0:1, :], (ROWS, 128)).T
    rk = jnp.broadcast_to(rs[1:2, :], (ROWS, 128)).T
    cos, sin = tab[0], tab[1]

    gq32r, gk32r = pltpu.roll(gq32, 64, axis=1), pltpu.roll(gk32, 64, axis=1)

    def rope(w, h, r, g, gr):
        cols = slice(h * 128, (h + 1) * 128)
        return (acc[w, :, cols] * r * g[h:h + 1] * cos + rolled[w, :, cols] * r * gr[h:h + 1] * sin).astype(BF16)

    ri = lax.broadcasted_iota(jnp.int32, (ROWS, ROWS), 0)
    ci = lax.broadcasted_iota(jnp.int32, (ROWS, ROWS), 1)
    same = (ri < SEQ) == (ci < SEQ)
    limit = jnp.where(ci < SEQ, lens[0], lens[1] + SEQ)
    allowed = same & (ci <= ri) & (ci < limit)
    for h in range(HEADS):
        part[h // 4, :, h % 4 * 128:(h % 4 + 1) * 128] = rope(0, h, rq, gq32, gq32r)
        kh = rope(1, h, rk, gk32, gk32r)
        kout[0, h] = kh[:SEQ]
        kout[1, h] = kh[SEQ:]
    for h in range(HEADS):
        kh = jnp.concatenate([kout[0, h], kout[1, h]], axis=0)
        s = jnp.where(allowed, dot_t(part[h // 4, :, h % 4 * 128:(h % 4 + 1) * 128], kh) * HEAD_DIM ** -0.5, -1e30)
        e = jnp.exp(s - jnp.max(s, axis=1, keepdims=True))
        part[2 + h // 4, :, h % 4 * 128:(h % 4 + 1) * 128] = (e / jnp.sum(e, axis=1, keepdims=True)).astype(BF16)
    for h in range(HEADS):
        vh = jnp.concatenate([vout[0, h], vout[1, h]], axis=0)
        ob[:, h * 128:(h + 1) * 128] = dot(part[2 + h // 4, :, h % 4 * 128:(h % 4 + 1) * 128], vh).astype(BF16)

    def d_copy(ph, c):
        return pltpu.make_async_remote_copy(
            part.at[c, theirs, :], d2d.at[c], d_s, d_r.at[c],
            device_id={"tp": partner}, device_id_type=MESH)

    def x_copy(ph, c):
        return pltpu.make_async_remote_copy(
            xsend.at[c], xrecv.at[ph, c], x_s, x_r.at[ph, c],
            device_id={"tp": cross}, device_id_type=MESH)

    def cols_of(c):
        return pl.ds(pl.multiple_of(c * CW, CW), CW)

    def a_copy(ph, c):
        blk = full.at[mine, cols_of(c)]
        return pltpu.make_async_remote_copy(
            blk, blk, a_s, a_r.at[c],
            device_id={"tp": partner}, device_id_type=MESH)

    def put(ph, c, val):
        part[c] = val.astype(BF16)
        d_copy(ph, c).start()

    def relay(ph, c):
        d_copy(ph, c).wait_recv()
        xsend[c] = (part[c, mine, :].astype(F32) + d2d[c].astype(F32)).astype(BF16)
        x_copy(ph, c).start()

    def add_sq(rows, c):
        v = full[rows, cols_of(c)].astype(F32)
        v = v * v
        t = v[:, 0:128]
        for q in range(1, CW // 128):
            t = t + v[:, q * 128:(q + 1) * 128]
        ssq[rows, :] += t

    def finish_own(ph, c):
        x_copy(ph, c).wait_recv()
        s = xsend[c].astype(F32) + xrecv[ph, c].astype(F32)
        full[mine, cols_of(c)] = s.astype(BF16)
        a_copy(ph, c).start()
        add_sq(mine, c)

    def sent(ph):
        for sem in (d_s, x_s, a_s):
            pltpu.make_async_remote_copy(
                xsend, xrecv.at[ph], sem, x_r.at[ph, 0],
                device_id={"tp": cross}, device_id_type=MESH).wait_send()

    def finish_other(ph, c):
        a_copy(ph, c).wait_recv()
        add_sq(theirs, c)

    _ph('wo')
    ssq[...] = jnp.zeros_like(ssq)
    lag = 3
    for c in range(4):
        stream(12 + c).wait()
        for half in range(2):
            cc = 2 * c + half
            put(0, cc, dot(ob[...], slot(12 + c)[:, half * CW:(half + 1) * CW]))
            if cc >= lag:
                relay(0, cc - lag)

    _ph('xpose')
    @pl.loop(0, 2 * NTB)
    def _(j):
        gu_wait(j)
        s, m, n = lax.rem(j, NS), j // NTB, lax.rem(j, NTB)
        cols = pl.ds(pl.multiple_of(n * TB, TB), TB)
        for k in range(D // TB):
            blk = stg[s, :, k * TB:(k + 1) * TB]
            if k % 2 == 0:
                t = blk.T
            else:
                t = dot_t(eye[...], blk).astype(BF16)
            wgu[m, k * TB:(k + 1) * TB, cols] = t

        @pl.when(j + NS < 2 * NTB)
        def _():
            gu_start(j + NS)

        @pl.when(j < lag)
        def _():
            relay(0, NC - lag + j)

        @pl.when((j >= 6) & (lax.rem(j, 2) == 0))
        def _():
            finish_own(0, (j - 6) // 2)

        @pl.when((j >= 9) & (lax.rem(j, 2) == 1))
        def _():
            finish_other(0, (j - 9) // 2)

    finish_other(0, NC - 1)
    sent(0)

    _ph('norm1')
    rs1 = row_scale(ssq)

    for c in range(NC):
        add_norm(xh, full, rs1, ga32, c)


    def gate_up(start, width, keep):
        g = dot(xh[:, :D], wgu[0, :, pl.ds(start, width)])
        u = dot(xh[:, :D], wgu[1, :, pl.ds(start, width)])
        v = (g * jax.nn.sigmoid(g) * u).astype(BF16)
        act[:, pl.ds(start, keep)] = v[:, :keep]

    for n in range(FF // NT):
        gate_up(n * NT, NT, NT)
        if n < NC // 2:
            down_copy(2 * n).start()
            down_copy(2 * n + 1).start()

    tail = FF // NT * NT
    gate_up(tail, FFP - tail, FF - tail)
    ssq[...] = jnp.zeros_like(ssq)

    _ph('down')
    lag2 = 2
    for c in range(NC):
        down_copy(c).wait()
        put(1, c, dot(act[...], wgu[c % 2, :FFP, c // 2 * CW:(c // 2 + 1) * CW]))
        if c >= lag2:
            relay(1, c - lag2)

    _ph('relay_tail')
    for cc in range(NC - lag2, NC):
        relay(1, cc)

    _ph('finish2')
    @pl.loop(0, NC)
    def _(c):
        finish_own(1, c)

        @pl.when(c > 0)
        def _():
            finish_other(1, c - 1)

    finish_other(1, NC - 1)
    sent(1)
    _ph('end')


def store_kernel(h, m, ssq, g32, kc, vc, y_h, kc_h, vc_h, y, sem):
    kv = [pltpu.make_async_copy(a, b, sem.at[i]) for i, (a, b) in enumerate(((kc, kc_h), (vc, vc_h)))]
    for copy in kv:
        copy.start()
    rs = row_scale(ssq)
    blocks = []
    for c in range(NC):
        for q in range(CW // 128):
            cols = slice(c * CW + q * 128, c * CW + (q + 1) * 128)
            r = c * (CW // 128) + q
            v = m[:, cols].astype(F32) * rs * g32[r:r + 1, :]
            y[:, cols] = (h[:, cols].astype(F32) + v).astype(BF16)
        cols = pl.ds(c * CW, CW)
        blocks.append(pltpu.make_async_copy(y.at[:, cols], y_h.at[:, cols], sem.at[2 + c]))
        blocks[-1].start()
    for copy in kv + blocks:
        copy.wait()


def solution(mesh):
    tables = rope_tables()

    def local_layer(tokens, seq_lens, w_q, w_k, w_v, w_o, g_q, g_k, g_attn, g_mlp, w_gate, w_up, w_down):
        vmem = pl.BlockSpec(memory_space=pltpu.VMEM)
        anyspace = pl.BlockSpec(memory_space=pl.ANY)
        dma = pltpu.SemaphoreType.DMA
        outs = pl.pallas_call(
            kernel,
            out_shape=(
                pltpu.VMEM((ROWS, DW), BF16),
                pltpu.VMEM((ROWS, D), BF16),
                pltpu.VMEM((ROWS, 128), F32),
                pltpu.VMEM((D // 128, 128), F32),
                pltpu.VMEM((PROMPTS, HEADS, SEQ, HEAD_DIM), BF16),
                pltpu.VMEM((PROMPTS, HEADS, SEQ, HEAD_DIM), BF16),
            ),
            in_specs=[anyspace] * 14,
            out_specs=(vmem,) * 6,
            scratch_shapes=[
                pltpu.VMEM((NS, TB, D), BF16),
                pltpu.VMEM((2, D, FFW), BF16),
                pltpu.VMEM((3, ROWS, QW), F32),
                pltpu.VMEM((ROWS, QW), BF16),
                pltpu.VMEM((NC, ROWS, CW), BF16),
                pltpu.VMEM((NC, HALF, CW), BF16),
                pltpu.VMEM((NC, HALF, CW), BF16),
                pltpu.VMEM((2, NC, HALF, CW), BF16),
                pltpu.VMEM((ROWS, FFP), BF16),
                pltpu.VMEM((2, ROWS, HEAD_DIM), F32),
                pltpu.VMEM((QW // 128, 128), BF16),
                pltpu.VMEM((QW // 128, 128), BF16),
                pltpu.VMEM((D // 128, 128), BF16),
                pltpu.VMEM((D // 128, 128), BF16),
                pltpu.VMEM((D // 128, 128), F32),
                pltpu.VMEM((8, 128), F32),
                pltpu.VMEM((3, 8, 128), F32),
                pltpu.VMEM((TB, TB), BF16),
                pltpu.SMEM((PROMPTS,), jnp.int32),
                pltpu.VMEM((2, ROWS, QW), F32),
                dma((11,)), dma((3,)), dma((3,)),
                dma, dma((NC,)), dma, dma((2, NC)), dma, dma((NC,)),
            ],
            compiler_params=pltpu.CompilerParams(
                collective_id=0, has_side_effects=True, vmem_limit_bytes=VMEM_LIMIT),
            name="layer",
        )(seq_lens, tokens.reshape(ROWS, D), w_q, w_k, w_v, w_o,
          g_q.reshape(-1, 128), g_k.reshape(-1, 128), g_attn.reshape(-1, 128), g_mlp.reshape(-1, 128),
          w_gate.T, w_up.T, w_down, jnp.asarray(tables))
        outs = [pltpu.with_memory_space_constraint(o, pltpu.VMEM) for o in outs]
        y, kc, vc = pl.pallas_call(
            store_kernel,
            out_shape=(
                jax.ShapeDtypeStruct((ROWS, D), BF16),
                jax.ShapeDtypeStruct((PROMPTS, HEADS, SEQ, HEAD_DIM), BF16),
                jax.ShapeDtypeStruct((PROMPTS, HEADS, SEQ, HEAD_DIM), BF16),
            ),
            in_specs=[vmem] * 6,
            out_specs=(anyspace,) * 3,
            scratch_shapes=[pltpu.VMEM((ROWS, D), BF16), dma((2 + NC,))],
            compiler_params=pltpu.CompilerParams(vmem_limit_bytes=3 * 2**19),
            name="store",
        )(*outs)
        return y.reshape(tokens.shape), kc, vc

    return jax.shard_map(local_layer, mesh=mesh, in_specs=(P('dp', None, None), P('dp'), P(None, 'tp'), P(None, 'tp'), P(None, 'tp'), P('tp', None), P('tp'), P('tp'), P(), P(), P(None, 'tp'), P(None, 'tp'), P('tp', None)), out_specs=(P('dp', None, None), P('dp', 'tp', None, None), P('dp', 'tp', None, None)), check_vma=False)
```

```python
import functools

import jax
import jax.numpy as jnp
import numpy as np
from jax import lax
from jax.experimental import pallas as pl
from jax.experimental.pallas import tpu as pltpu
from jax.sharding import PartitionSpec as P

HEAD_DIM = 128
ROPE_BASE = 500000.0
NORM_EPS = 1e-6

SEQ = 64
PROMPTS = 2
ROWS = SEQ * PROMPTS
HALF = ROWS // 2
D = 4096
QW = 1024
HEADS = QW // HEAD_DIM
FF = 2752
FFP = 2816
FFW = FFP + 128
DW = D + 128
KC = 1024
CW = 512
NC = D // CW
TB = 256
NTB = FFP // TB
NS = 4
DEPTH = 4
NEXT = {i: (i + 4,) for i in range(8)}
NEXT.update({9: (12,), 10: (13,), 11: (14, 15)})
NT = 512

VMEM_LIMIT = 61 * 2**20

F32 = jnp.float32
BF16 = jnp.bfloat16
MESH = pl.DeviceIdType.MESH


def rope_tables():
    half = HEAD_DIM // 2
    inv_freq = ROPE_BASE ** (-2.0 * np.arange(half, dtype=np.float64) / HEAD_DIM)
    inv_freq = inv_freq.astype(np.float32)
    angles = np.arange(SEQ, dtype=np.float32)[:, None] * inv_freq[None, :]
    cos = np.cos(angles.astype(np.float64)).astype(np.float32)
    sin = np.sin(angles.astype(np.float64)).astype(np.float32)
    cos2 = np.concatenate([cos, cos], axis=1)
    sin2 = np.concatenate([-sin, sin], axis=1)
    return np.stack([np.tile(cos2, (PROMPTS, 1)), np.tile(sin2, (PROMPTS, 1))])


def dot(a, b):
    return jnp.dot(a, b, preferred_element_type=F32)


def dot_t(a, b):
    return lax.dot_general(a, b, (((1,), (1,)), ((), ())), preferred_element_type=F32)


def row_scale(ssq):
    return lax.rsqrt(jnp.sum(ssq[...], axis=1, keepdims=True) * (1.0 / D) + NORM_EPS)


def add_norm(base, branch, rs, g32, c):
    for q in range(CW // 128):
        col = c * CW + q * 128
        cols = pl.ds(col if isinstance(c, int) else pl.multiple_of(col, 128), 128)
        v = branch[:, cols].astype(F32) * rs * g32[pl.ds(c * (CW // 128) + q, 1), :]
        base[:, cols] = (base[:, cols].astype(F32) + v).astype(BF16)


def kernel(lens_h, tok, wq, wk, wv, wo, gq_h, gk_h, ga_h, gm_h, wg, wu, wd, tab_h,
           xh, full, ssq, gm32, kout, vout,
           stg, wgu, acc, ob, part, d2d, xsend, xrecv, act,
           tab, gq, gk, ga, gm, ga32, st, st_recv, eye, lens, rolled,
           sem_w, st_s, st_r,
           d_s, d_r, x_s, x_r, a_s, a_r):
    me = lax.axis_index("tp")
    core = lax.rem(me, 2)
    partner = me + 1 - 2 * core
    cross = lax.rem(me + 2, 4)
    mine = pl.ds(pl.multiple_of(core * HALF, HALF), HALF)
    theirs = pl.ds(pl.multiple_of((1 - core) * HALF, HALF), HALF)
    local = pltpu.make_async_copy

    small = [(tok, xh.at[:, pl.ds(0, D)]), (tab_h, tab), (gq_h, gq), (gk_h, gk), (ga_h, ga), (gm_h, gm), (lens_h, lens)]

    def in_copy(i):
        return local(small[i][0], small[i][1], sem_w.at[4 + i])

    def slot(i):
        i = i % 8
        return wgu.at[1, pl.ds((i % 4) * KC, KC), pl.ds((i // 4) * KC, KC)]

    qkv = [wq, wk, wv]

    def stream(i):
        if i < 12:
            src = qkv[i // 4].at[pl.ds((i % 4) * KC, KC), :]
        else:
            src = wo.at[:, pl.ds((i - 12) * KC, KC)]
        return local(src, slot(i), sem_w.at[i % DEPTH])

    def gu_copy(w, n, s):
        rows = TB if n < NTB - 1 else FF - TB * (NTB - 1)
        return local(w.at[pl.ds(n * TB, rows), :], stg.at[s, pl.ds(0, rows), :], sem_w.at[4 + s])

    def gu_start(j):
        s = lax.rem(j, NS)
        n = lax.rem(j, NTB)
        for m, w in enumerate((wg, wu)):
            @pl.when((j // NTB == m) & (n < NTB - 1))
            def _():
                rows = pl.ds(pl.multiple_of(n * TB, TB), TB)
                local(w.at[rows, :], stg.at[s], sem_w.at[4 + s]).start()

            @pl.when((j // NTB == m) & (n == NTB - 1))
            def _():
                gu_copy(w, NTB - 1, s).start()

    def gu_wait(j):
        s = lax.rem(j, NS)
        n = lax.rem(j, NTB)

        @pl.when(n < NTB - 1)
        def _():
            gu_copy(wg, 0, s).wait()

        @pl.when(n == NTB - 1)
        def _():
            gu_copy(wg, NTB - 1, s).wait()

    def down_copy(c):
        return local(wd.at[:, pl.ds(c * CW, CW)],
                     wgu.at[c % 2, pl.ds(0, FF), pl.ds(c // 2 * CW, CW)], sem_w.at[c])

    in_copy(0).start()
    stream(0).start()
    for i in range(1, 7):
        in_copy(i).start()
    for i in range(1, DEPTH):
        stream(i).start()

    barrier = pltpu.get_barrier_semaphore()
    for j in range(1, 4):
        pl.semaphore_signal(barrier, inc=1, device_id={"tp": lax.rem(me + j, 4)}, device_id_type=MESH)
    acc[...] = jnp.zeros_like(acc)
    st[...] = jnp.zeros_like(st)
    er = lax.broadcasted_iota(jnp.int32, (TB, TB), 0)
    ec = lax.broadcasted_iota(jnp.int32, (TB, TB), 1)
    eye[...] = (er == ec).astype(F32).astype(BF16)
    act[:, FF // 128 * 128:] = jnp.zeros((ROWS, FFP - FF // 128 * 128), BF16)
    in_copy(0).wait()

    def qkv_step(i):
        stream(i).wait()
        w, k = i // 4, i % 4
        acc[w] += dot(xh[:, k * KC:(k + 1) * KC], slot(i)[...])
        for n in NEXT.get(i, ()):
            stream(n).start()

    for i in range(8):
        qkv_step(i)
    for w in range(2):
        t = jnp.zeros((ROWS, 128), F32)
        for h in range(HEADS):
            v = acc[w, :, h * 128:(h + 1) * 128]
            t = t + v * v
        st[w:w + 1, :] = jnp.sum(t.T, axis=0, keepdims=True)
    pl.semaphore_wait(barrier, 3)

    def st_copy(j):
        return pltpu.make_async_remote_copy(
            st, st_recv.at[j - 1], st_s.at[j - 1], st_r.at[j - 1],
            device_id={"tp": lax.rem(me + j, 4)}, device_id_type=MESH)

    for j in range(1, 4):
        st_copy(j).start()
    qkv_step(8)
    for w in range(2):
        for h in range(HEADS):
            cols = slice(h * 128, (h + 1) * 128)
            rolled[w, :, cols] = pltpu.roll(acc[w, :, cols], 64, axis=1)
    for i in range(9, 12):
        qkv_step(i)
    for i in range(1, 7):
        in_copy(i).wait()
    for j in range(NS):
        gu_copy(wg, j, j).start()
    ga32[...] = ga[...].astype(F32)
    gm32[...] = gm[...].astype(F32)
    gq32, gk32 = gq[...].astype(F32), gk[...].astype(F32)
    for h in range(HEADS):
        vh = acc[2, :, h * 128:(h + 1) * 128].astype(BF16)
        vout[0, h] = vh[:SEQ]
        vout[1, h] = vh[SEQ:]
    for j in range(1, 4):
        st_copy(j).wait()

    tot = st[...] + st_recv[0] + st_recv[1] + st_recv[2]
    rs = lax.rsqrt(tot * (1.0 / D) + NORM_EPS)
    rq = jnp.broadcast_to(rs[0:1, :], (ROWS, 128)).T
    rk = jnp.broadcast_to(rs[1:2, :], (ROWS, 128)).T
    cos, sin = tab[0], tab[1]

    gq32r, gk32r = pltpu.roll(gq32, 64, axis=1), pltpu.roll(gk32, 64, axis=1)

    def rope(w, h, r, g, gr):
        cols = slice(h * 128, (h + 1) * 128)
        return (acc[w, :, cols] * r * g[h:h + 1] * cos + rolled[w, :, cols] * r * gr[h:h + 1] * sin).astype(BF16)

    ri = lax.broadcasted_iota(jnp.int32, (ROWS, ROWS), 0)
    ci = lax.broadcasted_iota(jnp.int32, (ROWS, ROWS), 1)
    same = (ri < SEQ) == (ci < SEQ)
    limit = jnp.where(ci < SEQ, lens[0], lens[1] + SEQ)
    allowed = same & (ci <= ri) & (ci < limit)
    for h in range(HEADS):
        part[h // 4, :, h % 4 * 128:(h % 4 + 1) * 128] = rope(0, h, rq, gq32, gq32r)
        kh = rope(1, h, rk, gk32, gk32r)
        kout[0, h] = kh[:SEQ]
        kout[1, h] = kh[SEQ:]
    for h in range(HEADS):
        kh = jnp.concatenate([kout[0, h], kout[1, h]], axis=0)
        s = jnp.where(allowed, dot_t(part[h // 4, :, h % 4 * 128:(h % 4 + 1) * 128], kh) * HEAD_DIM ** -0.5, -1e30)
        e = jnp.exp(s - jnp.max(s, axis=1, keepdims=True))
        part[2 + h // 4, :, h % 4 * 128:(h % 4 + 1) * 128] = (e / jnp.sum(e, axis=1, keepdims=True)).astype(BF16)
    for h in range(HEADS):
        vh = jnp.concatenate([vout[0, h], vout[1, h]], axis=0)
        ob[:, h * 128:(h + 1) * 128] = dot(part[2 + h // 4, :, h % 4 * 128:(h % 4 + 1) * 128], vh).astype(BF16)

    def d_copy(ph, c):
        return pltpu.make_async_remote_copy(
            part.at[c, theirs, :], d2d.at[c], d_s, d_r.at[c],
            device_id={"tp": partner}, device_id_type=MESH)

    def x_copy(ph, c):
        return pltpu.make_async_remote_copy(
            xsend.at[c], xrecv.at[ph, c], x_s, x_r.at[ph, c],
            device_id={"tp": cross}, device_id_type=MESH)

    def cols_of(c):
        return pl.ds(pl.multiple_of(c * CW, CW), CW)

    def a_copy(ph, c):
        blk = full.at[mine, cols_of(c)]
        return pltpu.make_async_remote_copy(
            blk, blk, a_s, a_r.at[c],
            device_id={"tp": partner}, device_id_type=MESH)

    def put(ph, c, val):
        part[c] = val.astype(BF16)
        d_copy(ph, c).start()

    def relay(ph, c):
        d_copy(ph, c).wait_recv()
        xsend[c] = (part[c, mine, :].astype(F32) + d2d[c].astype(F32)).astype(BF16)
        x_copy(ph, c).start()

    def add_sq(rows, c):
        v = full[rows, cols_of(c)].astype(F32)
        v = v * v
        t = v[:, 0:128]
        for q in range(1, CW // 128):
            t = t + v[:, q * 128:(q + 1) * 128]
        ssq[rows, :] += t

    def finish_own(ph, c):
        x_copy(ph, c).wait_recv()
        s = xsend[c].astype(F32) + xrecv[ph, c].astype(F32)
        full[mine, cols_of(c)] = s.astype(BF16)
        a_copy(ph, c).start()
        add_sq(mine, c)

    def sent(ph):
        for sem in (d_s, x_s, a_s):
            pltpu.make_async_remote_copy(
                xsend, xrecv.at[ph], sem, x_r.at[ph, 0],
                device_id={"tp": cross}, device_id_type=MESH).wait_send()

    def finish_other(ph, c):
        a_copy(ph, c).wait_recv()
        add_sq(theirs, c)

    ssq[...] = jnp.zeros_like(ssq)
    lag = 3
    for c in range(4):
        stream(12 + c).wait()
        for half in range(2):
            cc = 2 * c + half
            put(0, cc, dot(ob[...], slot(12 + c)[:, half * CW:(half + 1) * CW]))
            if cc >= lag:
                relay(0, cc - lag)

    @pl.loop(0, 2 * NTB)
    def _(j):
        gu_wait(j)
        s, m, n = lax.rem(j, NS), j // NTB, lax.rem(j, NTB)
        cols = pl.ds(pl.multiple_of(n * TB, TB), TB)
        for k in range(D // TB):
            blk = stg[s, :, k * TB:(k + 1) * TB]
            if k % 2 == 0:
                t = blk.T
            else:
                t = dot_t(eye[...], blk).astype(BF16)
            wgu[m, k * TB:(k + 1) * TB, cols] = t

        @pl.when(j + NS < 2 * NTB)
        def _():
            gu_start(j + NS)

        @pl.when(j < lag)
        def _():
            relay(0, NC - lag + j)

        @pl.when((j >= 6) & (lax.rem(j, 2) == 0))
        def _():
            finish_own(0, (j - 6) // 2)

        @pl.when((j >= 9) & (lax.rem(j, 2) == 1))
        def _():
            finish_other(0, (j - 9) // 2)

    finish_other(0, NC - 1)
    sent(0)

    rs1 = row_scale(ssq)

    for c in range(NC):
        add_norm(xh, full, rs1, ga32, c)


    def gate_up(start, width, keep):
        g = dot(xh[:, :D], wgu[0, :, pl.ds(start, width)])
        u = dot(xh[:, :D], wgu[1, :, pl.ds(start, width)])
        v = (g * jax.nn.sigmoid(g) * u).astype(BF16)
        act[:, pl.ds(start, keep)] = v[:, :keep]

    for n in range(FF // NT):
        gate_up(n * NT, NT, NT)
        if n < NC // 2:
            down_copy(2 * n).start()
            down_copy(2 * n + 1).start()

    tail = FF // NT * NT
    gate_up(tail, FFP - tail, FF - tail)
    ssq[...] = jnp.zeros_like(ssq)

    lag2 = 2
    for c in range(NC):
        down_copy(c).wait()
        put(1, c, dot(act[...], wgu[c % 2, :FFP, c // 2 * CW:(c // 2 + 1) * CW]))
        if c >= lag2:
            relay(1, c - lag2)

    for cc in range(NC - lag2, NC):
        relay(1, cc)

    @pl.loop(0, NC)
    def _(c):
        finish_own(1, c)

        @pl.when(c > 0)
        def _():
            finish_other(1, c - 1)

    finish_other(1, NC - 1)
    sent(1)


def store_kernel(h, m, ssq, g32, kc, vc, y_h, kc_h, vc_h, y, sem):
    kv = [pltpu.make_async_copy(a, b, sem.at[i]) for i, (a, b) in enumerate(((kc, kc_h), (vc, vc_h)))]
    for copy in kv:
        copy.start()
    rs = row_scale(ssq)
    blocks = []
    for c in range(NC):
        for q in range(CW // 128):
            cols = slice(c * CW + q * 128, c * CW + (q + 1) * 128)
            r = c * (CW // 128) + q
            v = m[:, cols].astype(F32) * rs * g32[r:r + 1, :]
            y[:, cols] = (h[:, cols].astype(F32) + v).astype(BF16)
        cols = pl.ds(c * CW, CW)
        blocks.append(pltpu.make_async_copy(y.at[:, cols], y_h.at[:, cols], sem.at[2 + c]))
        blocks[-1].start()
    for copy in kv + blocks:
        copy.wait()


def solution(mesh):
    tables = rope_tables()

    def local_layer(tokens, seq_lens, w_q, w_k, w_v, w_o, g_q, g_k, g_attn, g_mlp, w_gate, w_up, w_down):
        vmem = pl.BlockSpec(memory_space=pltpu.VMEM)
        anyspace = pl.BlockSpec(memory_space=pl.ANY)
        dma = pltpu.SemaphoreType.DMA
        outs = pl.pallas_call(
            kernel,
            out_shape=(
                pltpu.VMEM((ROWS, DW), BF16),
                pltpu.VMEM((ROWS, D), BF16),
                pltpu.VMEM((ROWS, 128), F32),
                pltpu.VMEM((D // 128, 128), F32),
                pltpu.VMEM((PROMPTS, HEADS, SEQ, HEAD_DIM), BF16),
                pltpu.VMEM((PROMPTS, HEADS, SEQ, HEAD_DIM), BF16),
            ),
            in_specs=[anyspace] * 14,
            out_specs=(vmem,) * 6,
            scratch_shapes=[
                pltpu.VMEM((NS, TB, D), BF16),
                pltpu.VMEM((2, D, FFW), BF16),
                pltpu.VMEM((3, ROWS, QW), F32),
                pltpu.VMEM((ROWS, QW), BF16),
                pltpu.VMEM((NC, ROWS, CW), BF16),
                pltpu.VMEM((NC, HALF, CW), BF16),
                pltpu.VMEM((NC, HALF, CW), BF16),
                pltpu.VMEM((2, NC, HALF, CW), BF16),
                pltpu.VMEM((ROWS, FFP), BF16),
                pltpu.VMEM((2, ROWS, HEAD_DIM), F32),
                pltpu.VMEM((QW // 128, 128), BF16),
                pltpu.VMEM((QW // 128, 128), BF16),
                pltpu.VMEM((D // 128, 128), BF16),
                pltpu.VMEM((D // 128, 128), BF16),
                pltpu.VMEM((D // 128, 128), F32),
                pltpu.VMEM((8, 128), F32),
                pltpu.VMEM((3, 8, 128), F32),
                pltpu.VMEM((TB, TB), BF16),
                pltpu.SMEM((PROMPTS,), jnp.int32),
                pltpu.VMEM((2, ROWS, QW), F32),
                dma((11,)), dma((3,)), dma((3,)),
                dma, dma((NC,)), dma, dma((2, NC)), dma, dma((NC,)),
            ],
            compiler_params=pltpu.CompilerParams(
                collective_id=0, has_side_effects=True, vmem_limit_bytes=VMEM_LIMIT),
            name="layer",
        )(seq_lens, tokens.reshape(ROWS, D), w_q, w_k, w_v, w_o,
          g_q.reshape(-1, 128), g_k.reshape(-1, 128), g_attn.reshape(-1, 128), g_mlp.reshape(-1, 128),
          w_gate.T, w_up.T, w_down, jnp.asarray(tables))
        outs = [pltpu.with_memory_space_constraint(o, pltpu.VMEM) for o in outs]
        y, kc, vc = pl.pallas_call(
            store_kernel,
            out_shape=(
                jax.ShapeDtypeStruct((ROWS, D), BF16),
                jax.ShapeDtypeStruct((PROMPTS, HEADS, SEQ, HEAD_DIM), BF16),
                jax.ShapeDtypeStruct((PROMPTS, HEADS, SEQ, HEAD_DIM), BF16),
            ),
            in_specs=[vmem] * 6,
            out_specs=(anyspace,) * 3,
            scratch_shapes=[pltpu.VMEM((ROWS, D), BF16), dma((2 + NC,))],
            compiler_params=pltpu.CompilerParams(vmem_limit_bytes=3 * 2**19),
            name="store",
        )(*outs)
        return y.reshape(tokens.shape), kc, vc

    return jax.shard_map(local_layer, mesh=mesh, in_specs=(P('dp', None, None), P('dp'), P(None, 'tp'), P(None, 'tp'), P(None, 'tp'), P('tp', None), P('tp'), P('tp'), P(), P(), P(None, 'tp'), P(None, 'tp'), P('tp', None)), out_specs=(P('dp', None, None), P('dp', 'tp', None, None), P('dp', 'tp', None, None)), check_vma=False)
```
